32 devices in a mesh: lag: 2 (over core), space: 16 (over z, y, x).
Axes of the slice: x: 2, y: 2, z: 4, core: 2. Of those that a mesh axis runs over, the one named last changes fastest.
Arguments:
- ensemble: bfloat16 [2, 64, 65536], P('lag', None, 'space'), may hold values from -6 to 6
- obs_pert: bfloat16 [2, 64, 16384], P('lag', None, 'space'), may hold values from -6 to 6
- obs_innov: bfloat16 [2, 16384], P('lag', 'space'), may hold values from -12 to 12
- obs_rinv: bfloat16 [2, 16384], P('lag', 'space'), may hold values from 0.019897461 to 0.5
- obs_tile: int32 [2, 16384, 1], P('lag', 'space'), may hold values from 0 to 15; in each aligned block of 1024 rows (0 to 1023, 1024 to 2047, ..., all dimensions but the last counted through in order) at most 128 rows name the same one
- obs_column: int32 [2, 16384], P('lag', 'space'), may hold values from 0 to 4095
- obs_count: int32 [2, 16], P('lag', 'space'), may hold values from 512 to 1024, as said below
Outputs:
- analysis: bfloat16 [2, 64, 65536], P('lag', None, 'space')
The draws below stay inside these ranges and needn't reach their ends.
Inputs may be any that keep to these rules, and one draw needn't show every extreme that they name: `obs_tile`: among the 1024 slots of one device at one lag, no tile is named more than 128 times. `obs_count`: slots of a device past its count are not used; in every draw some device uses all 1024.
All inputs are finite; a program needn't handle non-finite values.
Results may differ from the reference program's by a relative error of at most 0.0022.
The reference program's roundings to bfloat16 on the way count: a program that leaves them out, or rounds other values in their place, can miss the bound.
Values may be sent and summed in bfloat16 or wider, within the bound.
A program may use at most 64 MiB of HBM per device.

```python
import math
import jax
import jax.numpy as jnp
import numpy as np
from jax import lax

MEMBERS = 64
COLS_DEV = 4096
SPACING = 512
OBS_DEV = 1024
NS_ITERS = 6
TILES = 16
LAGS = 2
NCOLS = 65536
OBS = 16384
PTS = 8
NPTS = 128
RADIUS = 2048
SLOT = 128
RECV = 2048


def draw_obs_count(key, part):
    base = jax.random.randint(jax.random.fold_in(key, 11), (LAGS, TILES), OBS_DEV // 2, OBS_DEV + 1)
    chosen = jax.random.randint(jax.random.fold_in(key, 12), (), 0, LAGS * TILES)
    flat = base.reshape(-1)
    flat = jnp.where(jnp.arange(LAGS * TILES) == chosen, OBS_DEV, flat)
    return flat.reshape(LAGS, TILES).astype(jnp.int32)


def touch_ends(values, own_key, least, top_value):
    longest = values.shape.index(max(values.shape))
    spots = []
    for shift in (0, 1):
        where = [jax.random.randint(jax.random.fold_in(own_key, axis), (), 0, length) for axis, length in enumerate(values.shape)]
        where[longest] = (where[longest] + shift) % values.shape[longest]
        spots.append(tuple(where))
    return values.at[spots[0]].set(least).at[spots[1]].set(top_value)


def steps_of(key, extent, shards, least, top_value):
    level = 1.0
    for position, blocks in shards:
        draws = jax.random.uniform(jax.random.fold_in(jax.random.fold_in(key, 6), position), (blocks,), jnp.float32, least / len(shards), top_value / len(shards))
        level = level * jnp.repeat(jnp.exp(draws), extent[position] // blocks).reshape((-1,) + (1,) * (len(extent) - 1 - position))
    return level


def shared_out(key, own, number, rows, amount, top, reach, lean):
    ranking = jax.random.permutation(key, amount)
    heavy_load, ordinary = shares(amount, rows * top, reach, lean, True), shares(amount, rows * top, reach, lean, False)
    places = jnp.arange(amount)

    def named(sizes, rotation):
        used = int((sizes > 0).sum())
        fixed = max(1, used // 4)
        passed = fixed + (places - fixed + rotation * (used - fixed)) % max(1, amount - fixed)
        return jnp.zeros((amount,), jnp.int32).at[ranking[jnp.where(places < fixed, places, passed)]].set(jnp.asarray(sizes, jnp.int32))

    sizes = jnp.where(number % 4 == 0, named(heavy_load, number // 4), named(ordinary, number - number // 4 - 1))
    mixed = jax.random.permutation(jax.random.fold_in(own, 3), amount)
    source_of, receiver = mixed[0:amount // 2 * 2:2], mixed[1:amount // 2 * 2:2]
    room = jnp.minimum(sizes[source_of] - 1, reach - sizes[receiver]) // 2
    room = jnp.where((source_of == ranking[0]) | (receiver == ranking[0]) | (sizes[receiver] == 0), 0, jnp.maximum(room, 0))
    passed = jax.random.randint(jax.random.fold_in(own, 4), (amount // 2,), 0, 1 << 20) % (room + 1)
    sizes = sizes.at[source_of].add(-passed).at[receiver].add(passed)
    items = jnp.searchsorted(jnp.cumsum(sizes), jnp.arange(rows * top), side="right").astype(jnp.int32)
    table = items.reshape(top, rows).T
    table = table[jax.random.permutation(jax.random.fold_in(own, 1), rows)]
    rotation = jax.random.randint(jax.random.fold_in(own, 2), (rows, 1), 0, top)
    return jnp.take_along_axis(table, (jnp.arange(top)[None, :] + rotation) % top, axis=1)


def shares(number_of, total, reach, skew, full):
    portions = [(1 << 20) // math.isqrt(rank ** skew) + 1 for rank in range(1, number_of + 1)]
    largest = reach if full else min(reach, max(-(-total // number_of), total * portions[0] // sum(portions)))
    least = 1 if total - largest >= number_of - 1 else 0
    given, rest = [largest] + [least] * (number_of - 1), total - largest - least * (number_of - 1)
    while rest > 0:
        movable = [i for i in range(1, number_of) if given[i] < largest] or [i for i in range(1, number_of) if given[i] < reach]
        pool, remaining = sum([portions[i] for i in movable]), rest
        for i in movable:
            more = min(reach - given[i], max(1, remaining * portions[i] // pool), rest)
            given[i] = given[i] + more
            rest = rest - more
    return np.array(given)


def centred(own_key, dims, width, limit, split=(), kind=jnp.bfloat16):
    result = jax.random.normal(own_key, dims, jnp.float32) * width
    if len(split) > 0:
        result = steps_of(own_key, dims, split, -0.22, 0.18) * result
    return jnp.clip(result, min=-limit, max=limit).astype(kind)


def setup_inputs(seed: int = 0) -> dict:
    key_of = jax.random.split(jax.random.key(seed), 8)
    ensemble = centred(key_of[0], (LAGS, MEMBERS, NCOLS), 1.0, 6.0, ((0, 2), (2, 16)))
    obs_pert = centred(key_of[1], (LAGS, MEMBERS, OBS), 1.0, 6.0, ((0, 2), (2, 16)))
    obs_innov = centred(key_of[2], (LAGS, OBS), 2.0, 12.0, ((0, 2), (1, 16)))
    obs_rinv = jnp.clip(jnp.exp(math.log(0.5) - 3.224016 * jax.random.uniform(key_of[3], (LAGS, OBS), jnp.float32) ** steps_of(key_of[3], (LAGS, OBS), ((0, 2), (1, 16)), -0.2, 0.2)), 0.019897461, 0.5).astype(jnp.bfloat16)
    obs_tile_keys = jax.random.split(jax.random.fold_in(key_of[4], 1), LAGS * OBS // OBS_DEV)
    obs_tile_turns = jax.random.permutation(jax.random.fold_in(key_of[4], 3), LAGS * OBS // OBS_DEV)
    obs_tile = jax.vmap(lambda own, number: shared_out(jax.random.fold_in(key_of[4], 2), own, number, OBS_DEV, TILES, 1, SLOT, 1))(obs_tile_keys, obs_tile_turns).reshape((LAGS, OBS, 1))
    obs_column = touch_ends(jax.random.randint(key_of[5], (LAGS, OBS), 0, COLS_DEV), jax.random.fold_in(key_of[5], 1), 0, COLS_DEV - 1).astype(jnp.int32)
    obs_count = draw_obs_count(jax.random.fold_in(key_of[7], 71), 0)
    return {"ensemble": ensemble, "obs_pert": obs_pert, "obs_innov": obs_innov, "obs_rinv": obs_rinv, "obs_tile": obs_tile, "obs_column": obs_column, "obs_count": obs_count}


def point_moments(centers, pert, weight, innov, places, radius):
    distance = jnp.abs(places[None, :] - centers[:, None])
    tapers = jnp.square(jnp.maximum(1.0 - distance / radius, 0.0)) * weight[None, :]
    scaled = (pert.astype(jnp.float32)[None] * tapers[:, None, :]).astype(jnp.bfloat16)
    gram_mats = jnp.einsum('gko,jo->gkj', scaled.astype(jnp.float32), pert.astype(jnp.float32))
    drive_vec = jnp.einsum('gko,o->gk', scaled.astype(jnp.float32), innov.astype(jnp.float32))
    return (gram_mats, drive_vec)

def chain_product(left_mats, right_mats):
    return jnp.einsum('pij,pjk->pik', left_mats, right_mats, precision=lax.Precision.HIGHEST)

def transform(gram_mats, drive_vec):
    identity = jnp.eye(MEMBERS, dtype=jnp.float32)
    gram_mats = gram_mats + (MEMBERS - 1.0) * identity
    norm_scale = jnp.sqrt(lax.optimization_barrier(jnp.sum(gram_mats * gram_mats, axis=(1, 2))))
    upper_iter = gram_mats / norm_scale[:, None, None]
    lower_iter = jnp.broadcast_to(identity, gram_mats.shape)
    for sweep in range(NS_ITERS):
        middle = 1.5 * identity - 0.5 * chain_product(lower_iter, upper_iter)
        upper_iter = chain_product(upper_iter, middle)
        lower_iter = chain_product(middle, lower_iter)
    inv_root = lower_iter / jnp.sqrt(norm_scale)[:, None, None]
    inner = jnp.einsum('pij,pj->pi', inv_root, drive_vec, precision=lax.Precision.HIGHEST)
    mean_shift = jnp.einsum('pij,pj->pi', inv_root, inner, precision=lax.Precision.HIGHEST)
    full_weights = math.sqrt(MEMBERS - 1.0) * inv_root + mean_shift[:, :, None]
    return full_weights - lax.optimization_barrier(jnp.mean(full_weights, axis=1, keepdims=True)) + 1.0 / MEMBERS

def reference(ensemble, obs_pert, obs_innov, obs_rinv, obs_tile, obs_column, obs_count):
    centers = (jnp.arange(PTS).astype(jnp.int32) * SPACING + SPACING // 2).astype(jnp.float32)
    offsets = jnp.repeat(jnp.array([-COLS_DEV, 0, COLS_DEV], dtype=jnp.int32), RECV)

    def lag_weights(inputs):
        pert, innov, rinv, tile, column, count = inputs
        slot_ids = jnp.arange(OBS).astype(jnp.int32)
        source = slot_ids // OBS_DEV
        is_valid = slot_ids % OBS_DEV < count[source]
        destination = tile[:, 0]
        dest_hits = (destination[:, None] == jnp.arange(TILES).astype(jnp.int32)[None, :]).astype(jnp.int32)
        dest_hits = dest_hits.reshape(TILES, OBS_DEV, TILES)
        before = jnp.cumsum(dest_hits, axis=1) - dest_hits
        rank = lax.optimization_barrier(jnp.sum(before * dest_hits, axis=2)).reshape(-1)
        placed = destination * RECV + source * SLOT + rank
        weight = jnp.where(is_valid, rinv, jnp.zeros_like(rinv))
        bucket_pert = jnp.zeros((MEMBERS, TILES * RECV), jnp.bfloat16).at[:, placed].set(pert)
        bucket_meta = jnp.zeros((2, TILES * RECV), jnp.bfloat16).at[:, placed].set(jnp.stack([weight, innov]))
        bucket_cols = jnp.zeros((TILES * RECV,), jnp.int32).at[placed].set(column)
        bucket_pert = bucket_pert.reshape(MEMBERS, TILES, RECV)
        bucket_meta = bucket_meta.reshape(2, TILES, RECV)
        bucket_cols = bucket_cols.reshape(TILES, RECV)

        def tile_weights(tile_index):
            chosen = (tile_index + jnp.arange(-1, 2).astype(jnp.int32)) % TILES
            window_pert = jnp.take(bucket_pert, chosen, axis=1).reshape(MEMBERS, 3 * RECV)
            window_meta = jnp.take(bucket_meta, chosen, axis=1).reshape(2, 3 * RECV)
            window_cols = jnp.take(bucket_cols, chosen, axis=0).reshape(-1)
            places = (window_cols + offsets).astype(jnp.float32)
            gram_mats, drive_vec = point_moments(centers, window_pert, window_meta[0].astype(jnp.float32), window_meta[1], places, RADIUS)
            return transform(gram_mats, drive_vec)
        per_tile = lax.map(tile_weights, jnp.arange(TILES).astype(jnp.int32))
        return per_tile.reshape(NPTS, MEMBERS, MEMBERS)
    weights = lax.map(lag_weights, (obs_pert, obs_innov, obs_rinv, obs_tile, obs_column, obs_count))
    identity = jnp.broadcast_to(jnp.eye(MEMBERS, dtype=jnp.float32), (NPTS, MEMBERS, MEMBERS))

    def suffix_step(product, factor):
        newer = chain_product(factor, product)
        return (newer, newer)
    last_carry, products = lax.scan(suffix_step, identity, weights, reverse=True)
    half_span = SPACING // 2
    offsets_in = jnp.arange(SPACING).astype(jnp.float32)
    weight_mid = 1.0 - jnp.abs(offsets_in - half_span) / SPACING
    weight_prev = 1.0 - (offsets_in[:half_span] + half_span) / SPACING
    weight_next = 1.0 - (SPACING + half_span - offsets_in[half_span:]) / SPACING

    def lag_apply(inputs):
        members_block, lag_products = inputs
        rounded = lag_products.astype(jnp.bfloat16).astype(jnp.float32)
        previous = jnp.roll(rounded, 1, axis=0)
        following = jnp.roll(rounded, -1, axis=0)
        blocks = members_block.astype(jnp.float32).reshape(MEMBERS, NPTS, SPACING)
        middle_part = jnp.einsum('jkm,kjo->mjo', rounded, blocks)
        lower_part = jnp.einsum('jkm,kjo->mjo', previous, blocks[:, :, :half_span])
        upper_part = jnp.einsum('jkm,kjo->mjo', following, blocks[:, :, half_span:])
        sides = jnp.concatenate([lower_part * weight_prev, upper_part * weight_next], axis=2)
        analysed = middle_part * weight_mid + sides
        return analysed.reshape(MEMBERS, NCOLS).astype(jnp.bfloat16)
    return lax.map(lag_apply, (ensemble, products))
```

```python
import functools
import math

import jax
import jax.numpy as jnp
from jax import lax
from jax.experimental import pallas as pl
from jax.experimental.pallas import tpu as pltpu
from jax.sharding import PartitionSpec as P

SPACING = 512
NS_ITERS = 6
AHEAD = 3
EDGE = 6
LIMIT = 24 * 1024 * 1024
LANES = 128
META = 16
BASE = 64
F32 = jnp.float32
BF16 = jnp.bfloat16
NT = (((1,), (1,)), ((), ()))


def halves(x):
    hi = x.astype(BF16)
    return hi, (x - hi.astype(F32)).astype(BF16)


def stationary(hi, lo):
    row = jnp.concatenate([hi, lo], axis=1)
    return jnp.concatenate([row, row], axis=0)


def times(left, weights):
    width = weights.shape[1] // 2
    hi, lo = halves(left)
    out = jnp.dot(jnp.concatenate([hi, lo], axis=1), weights, preferred_element_type=F32)
    return out[:, :width] + out[:, width:]


def partner(me, step, tiles):
    if tiles & (tiles - 1):
        return lax.rem(me + step, tiles)
    other, bit = me, 1
    while bit < tiles:
        if step & bit:
            other = other + bit - 2 * bit * lax.rem(lax.div(me, bit), 2)
        bit *= 2
    return other


def weights_kernel(
    tiles, lags, slots, group, columns,
    pert_hbm, innov_hbm, rinv_hbm, tile_hbm, col_hbm, count_hbm, ens_hbm,
    turned, ens,
    move_sem,
    innov_ref, rinv_ref, tile_ref, col_ref, count_ref, load_sem,
    msg, snd, rcv, acc, to_left, to_right, from_left, from_right, mine, theirs,
    a2a_send, a2a_recv, halo_send, halo_recv, lag_send, lag_recv, product, edge, edge_rcv, edge_acc, edge_send, edge_recv,
):
    members, own = pert_hbm.shape
    points = columns // SPACING
    half = points // 2
    radius = columns // 2
    pair = 2 * members
    sent = members + META // 2
    me = lax.axis_index("space")
    my_lag = lax.axis_index("lag")

    barrier = pltpu.get_barrier_semaphore()
    order = range(tiles - 1, 0, -1)
    for step in order:
        pl.semaphore_signal(barrier, inc=1, device_id={"space": partner(me, step, tiles)})
    for step in range(1, lags):
        pl.semaphore_signal(barrier, inc=1, device_id={"lag": lax.rem(my_lag + step, lags)})

    loads = [
        pltpu.make_async_copy(source, dest, load_sem.at[n])
        for n, (source, dest) in enumerate((
            (tile_hbm, tile_ref),
            (count_hbm, count_ref),
            (rinv_hbm, rinv_ref),
            (innov_hbm, innov_ref),
            (col_hbm, col_ref),
            (pert_hbm, msg.at[0:members]),
        ))
    ]
    for load in loads:
        load.start()
    for load in loads:
        load.wait()

    slot_id = lax.broadcasted_iota(jnp.int32, (1, own), 1)
    weight = jnp.where(slot_id < count_ref[0, 0], rinv_ref[...].astype(F32), 0.0)
    column = col_ref[...]
    col_hi = (column // BASE).astype(F32)
    col_lo = (column % BASE).astype(F32)
    row = lax.broadcasted_iota(jnp.int32, (META, own), 0)
    meta = jnp.where(row == 0, weight, 0.0)
    meta = jnp.where(row == 1, innov_ref[...].astype(F32), meta)
    meta = jnp.where(row == 2, col_hi, meta)
    meta = jnp.where(row == 3, col_lo, meta)
    msg[members:, :] = meta.astype(BF16)

    target = tile_ref[...]
    hits = jnp.where(target == lax.broadcasted_iota(jnp.int32, (tiles, own), 0), 1.0, 0.0)
    tri = jnp.where(
        lax.broadcasted_iota(jnp.int32, (LANES, LANES), 0)
        < lax.broadcasted_iota(jnp.int32, (LANES, LANES), 1),
        1.0, 0.0,
    ).astype(BF16)
    seen = jnp.zeros((tiles, 1), F32)
    ranks = []
    for b in range(own // LANES):
        block = hits[:, b * LANES : (b + 1) * LANES]
        ahead = jnp.dot(block.astype(BF16), tri, preferred_element_type=F32) + seen
        ranks.append(jnp.sum(ahead * block, axis=0, keepdims=True))
        seen = seen + jnp.sum(block, axis=1, keepdims=True)
    rank = jnp.concatenate(ranks, axis=1)
    place = lax.broadcasted_iota(jnp.int32, (slots, own), 0).astype(F32).astype(BF16)
    message = msg[...]

    def bucket(dest):
        wanted = jnp.where(target == dest, rank, -1.0).astype(BF16)
        chosen = jnp.where(place == wanted, jnp.ones((), BF16), jnp.zeros((), BF16))
        return lax.dot_general(message, chosen, NT, preferred_element_type=F32).astype(BF16)

    def a2a(step):
        return pltpu.make_async_remote_copy(
            src_ref=snd.at[step, 0:sent], dst_ref=rcv.at[step, 0:sent],
            send_sem=a2a_send.at[step], recv_sem=a2a_recv.at[step],
            device_id={"space": partner(me, step, tiles)},
        )

    def edge_copy(source):
        return pltpu.make_async_remote_copy(
            src_ref=edge.at[0:sent], dst_ref=edge_rcv.at[source, 0:sent],
            send_sem=edge_send.at[0], recv_sem=edge_recv.at[source],
            device_id={"space": 0 * me},
        )

    edge[...] = bucket(tiles - 1)
    for step in order[:AHEAD]:
        snd[step] = bucket(partner(me, step, tiles))
    pl.semaphore_wait(barrier, tiles - 1 + lags - 1)
    for n, step in enumerate(order):
        if n >= AHEAD:
            snd[step] = bucket(partner(me, step, tiles))
        if n == EDGE:
            @pl.when(me > 0)
            def _():
                edge_copy(me).start()
        if n >= AHEAD - 1:
            for early in order[0 if n == AHEAD - 1 else n - 1 : n] if n >= AHEAD else order[: AHEAD - 1]:
                a2a(early).start()
    a2a(order[-1]).start()
    rcv[0] = bucket(me)
    for step in order:
        rcv[step, sent:] = jnp.zeros((members + META - sent, slots), BF16)

    ens_load = pltpu.make_async_copy(ens_hbm, ens, move_sem.at[0])
    ens_load.start()
    arrivals = list(range(tiles))

    def partials(obs, ks, into, base, fresh):
        pert = obs[0:members].astype(F32)
        info = obs[members:].astype(F32)
        obs_weight = info[0:1]
        places = info[2:3] * BASE + info[3:4]
        for k in ks:
            center = float((k - half) * SPACING + SPACING // 2)
            taper = jnp.maximum(1.0 - jnp.abs(places - center) / radius, 0.0)
            rho = taper * taper * obs_weight
            scaled = (pert * rho).astype(BF16)
            part = lax.dot_general(scaled, obs, NT, preferred_element_type=F32)
            if fresh:
                into[k - base] = part
            else:
                into[k - base] += part

    for first in range(0, tiles, group):
        for step in arrivals[max(first, 1) : first + group]:
            a2a(step).wait_recv()
        obs = jnp.concatenate([rcv[step] for step in arrivals[first : first + group]], axis=1)

        def moments(ks, obs=obs, first=first):
            partials(obs, ks, acc, 0, first == 0)

        @pl.when(me == 0)
        def _(first=first):
            for step in arrivals[max(first, 1) : first + group]:
                edge_copy(step).wait_recv()
            near = [
                edge_rcv[step] if step else edge[...] for step in arrivals[first : first + group]
            ]
            partials(
                jnp.concatenate(near, axis=1), range(points + half - 1, points + 2 * half),
                edge_acc, points + half - 1, first == 0,
            )

        if first + group < tiles:
            moments(range(points + 2 * half))

    lane = lax.broadcasted_iota(jnp.int32, (members, pair), 1)
    low = lane < members

    def joined(a, b, source=acc):
        return jnp.concatenate([source[a, :, 0:members], source[b, :, 0:members]], axis=1)

    def drive_of(a, source=acc):
        return source[a, :, members + 1 : members + 2]

    left_copy = pltpu.make_async_remote_copy(
        src_ref=to_left, dst_ref=from_right, send_sem=halo_send.at[0], recv_sem=halo_recv.at[0],
        device_id={"space": lax.rem(me + tiles - 1, tiles)},
    )
    right_copy = pltpu.make_async_remote_copy(
        src_ref=to_right, dst_ref=from_left, send_sem=halo_send.at[1], recv_sem=halo_recv.at[1],
        device_id={"space": lax.rem(me + 1, tiles)},
    )

    fold = members // 2
    row = lax.broadcasted_iota(jnp.int32, (members, pair), 0)
    within = lax.rem(lane, members)
    strip = lax.broadcasted_iota(jnp.int32, (fold, pair), 1) - members

    def packed(single, ks, source=acc):
        first = [joined(ks[n], ks[n + 1], source) for n in range(0, half, 2)]
        columns = [drive_of(k, source) for k in sorted([single, *ks])]
        for other in first[1::2]:
            diag = jnp.where(row == within, other, 0.0)
            columns.append(jnp.sum(jnp.where(low, diag, 0.0), axis=1, keepdims=True))
            columns.append(jnp.sum(jnp.where(low, 0.0, diag), axis=1, keepdims=True))
        parts = [
            jnp.where(row <= within, first[n], first[n + 1]) for n in range(0, half // 2, 2)
        ]
        tail = jnp.concatenate(
            [source[single, 0:fold, 0:members], source[single, fold:members, 0:members]], axis=1
        )
        for n, column in enumerate(columns):
            tail = jnp.where(strip == 2 * n, column[0:fold], tail)
            tail = jnp.where(strip == 2 * n + 1, column[fold:], tail)
        return jnp.concatenate([*parts, tail], axis=0)

    def unpacked(ref):
        tail = ref[members * (half // 4) :]

        def column(n):
            return jnp.concatenate(
                [
                    tail[:, members + 2 * n : members + 2 * n + 1],
                    tail[:, members + 2 * n + 1 : members + 2 * n + 2],
                ],
                axis=0,
            )

        pairs = []
        for n in range(half // 4):
            part = ref[n * members : (n + 1) * members]
            turned_part = jnp.concatenate([part[:, 0:members].T, part[:, members:].T], axis=1)
            pairs.append(jnp.where(row <= within, part, turned_part))
            diag = jnp.where(low, column(half + 1 + 2 * n), column(half + 2 + 2 * n))
            other = jnp.where(row == within, diag, turned_part)
            pairs.append(jnp.where(row > within, part, other))
        corner = tail[:, 0:members].T[fold:]
        bottom = jnp.concatenate([corner, tail[:, members + fold :]], axis=1)
        single = jnp.concatenate([tail[:, 0:members], bottom], axis=0)
        return pairs, single, [column(n) for n in range(half + 1)]

    last = points + 2 * half - 1
    moments(range(half + 1))
    to_left[...] = packed(0, list(range(1, half + 1)))
    moments(range(last - half, last + 1))
    left_copy.start()
    to_right[...] = packed(last, list(range(last - half, last)))

    moments(range(half + 1, half + 3))

    @pl.when(me < tiles - 1)
    def _():
        right_copy.start()

    moments(range(half + 3, last - half))

    eye = jnp.where(
        lax.rem(lane, members) == lax.broadcasted_iota(jnp.int32, (members, pair), 0), 1.0, 0.0
    )
    mask_low = jnp.where(low, 1.0, 0.0).astype(BF16)
    mask_high = jnp.where(low, 0.0, 1.0).astype(BF16)

    def diagonal(x):
        return jnp.concatenate([x * mask_low, x * mask_high], axis=0)

    def blocks(x):
        hi, lo = halves(x)
        return stationary(diagonal(hi), diagonal(lo))


    count = (points + 2) // 2
    own_pairs = [joined(half - 1 + 2 * i, half + 2 * i) for i in range(count)]
    own_drives = [drive_of(half - 1 + j) for j in range(points + 2)]
    left_copy.wait_recv()

    @pl.when(me > 0)
    def _():
        right_copy.wait_recv()

    @pl.when(me == 0)
    def _():
        from_left[...] = packed(half, list(range(half)), edge_acc)

    lefts, left_single, left_drives = unpacked(from_left)
    rights, right_single, right_drives = unpacked(from_right)

    grams = []
    for i in range(count):
        total = own_pairs[i] + (members - 1.0) * eye
        if i < half // 2:
            total = total + lefts[i]
        elif i == half // 2:
            total = total + jnp.concatenate([left_single, right_single], axis=1)
        else:
            total = total + rights[i - half // 2 - 1]
        grams.append(total)
    drives = [
        own + other for own, other in zip(own_drives, [*left_drives, *right_drives])
    ]

    uppers, lowers, scales = [], [], []
    for total in grams:
        squares = jnp.sum(total * total, axis=0, keepdims=True)
        row_low = lax.broadcasted_iota(jnp.int32, (1, pair), 1) < members
        sum_low = jnp.sum(jnp.where(row_low, squares, 0.0), axis=1, keepdims=True)
        sum_high = jnp.sum(jnp.where(row_low, 0.0, squares), axis=1, keepdims=True)
        scale = jnp.sqrt(jnp.where(row_low, sum_low, sum_high))
        scales.append(scale)
        uppers.append(total / scale)

    for sweep in range(NS_ITERS):
        if sweep == 0:
            middles = [1.5 * eye - 0.5 * up for up in uppers]
            lowers = middles
            uppers = [times(up, blocks(mid)) for up, mid in zip(uppers, middles)]
        else:
            middles = [
                1.5 * eye - 0.5 * times(lo, blocks(up)) for lo, up in zip(lowers, uppers)
            ]
            if sweep < NS_ITERS - 1:
                both = [
                    times(jnp.concatenate([up, lo], axis=0), blocks(mid))
                    for up, lo, mid in zip(uppers, lowers, middles)
                ]
                uppers = [x[0:members] for x in both]
                lowers = [x[members:] for x in both]
            else:
                lowers = [times(lo, blocks(mid)) for lo, mid in zip(lowers, middles)]

    results = []
    for i in range(count):
        root = lowers[i] / jnp.sqrt(scales[i])
        top = jnp.where(low, drives[2 * i], 0.0)
        bottom = jnp.where(low, 0.0, drives[2 * i + 1])
        hi, lo = halves(jnp.concatenate([top, bottom], axis=0))
        inner = times(root, stationary(hi, lo))
        shift = times(root, blocks(inner))
        full = math.sqrt(members - 1.0) * root + shift
        results.append(full - jnp.mean(full, axis=0, keepdims=True) + 1.0 / members)
    for i in range(count):
        mine[i] = results[i]
        product[i] = results[i]

    def lag_copy(step):
        return pltpu.make_async_remote_copy(
            src_ref=mine, dst_ref=theirs.at[step - 1],
            send_sem=lag_send.at[step - 1], recv_sem=lag_recv.at[step - 1],
            device_id={"lag": lax.rem(my_lag + lags - step, lags)},
        )

    for step in range(1, lags):
        @pl.when(my_lag >= step)
        def _(step=step):
            lag_copy(step).start()
    for step in range(1, lags):
        @pl.when(my_lag + step < lags)
        def _(step=step):
            lag_copy(step).wait_recv()
            for i in range(count):
                product[i] = times(product[i], blocks(theirs[step - 1, i]))
    for i in range(count):
        turned[i * pair : (i + 1) * pair] = product[i].T.astype(BF16)
    ens_load.wait()

    for step in range(1, tiles):
        a2a(step).wait_send()
    left_copy.wait_send()

    @pl.when(me < tiles - 1)
    def _():
        right_copy.wait_send()

    @pl.when(me > 0)
    def _():
        edge_copy(me).wait_send()

    for step in range(1, lags):
        @pl.when(my_lag >= step)
        def _(step=step):
            lag_copy(step).wait_send()


def apply_kernel(turned, ens, out_hbm, out, store_sem):
    members, columns = ens.shape
    points = columns // SPACING
    stores = []
    half_span = SPACING // 2
    for s in range(points + 1):
        start = max(s * SPACING - half_span, 0)
        stop = min(s * SPACING + half_span, columns)
        both = jnp.dot(
            turned[s * members : (s + 2) * members], ens[:, start:stop],
            preferred_element_type=F32,
        )
        along = lax.broadcasted_iota(jnp.int32, (1, stop - start), 1).astype(F32)
        second = (along + float(start - (s * SPACING - half_span))) / SPACING
        mixed = both[0:members] * (1.0 - second) + both[members:] * second
        out[:, start:stop] = mixed.astype(BF16)
        if s % 3 == 2:
            first = max((s - 2) * SPACING - half_span, 0)
            store = pltpu.make_async_copy(
                out.at[:, first:stop], out_hbm.at[:, first:stop], store_sem.at[s // 3]
            )
            store.start()
            stores.append(store)
    for store in stores:
        store.wait()


def per_device(ensemble, obs_pert, obs_innov, obs_rinv, obs_tile, obs_column, obs_count):
    members, columns = ensemble.shape[1:]
    own = obs_pert.shape[2]
    tiles, lags = lax.axis_size("space"), lax.axis_size("lag")
    slot_size = max(2, 2 * own // tiles)
    slots = -(-slot_size // LANES) * LANES
    group = 4
    points = columns // SPACING
    half = points // 2
    count = (points + 2) // 2
    pair = 2 * members
    rows = members + META
    side = (members * (half // 4) + members // 2, pair)
    turned, held = pl.pallas_call(
        functools.partial(weights_kernel, tiles, lags, slots, group, columns),
        out_shape=(pltpu.VMEM((count * pair, members), BF16), pltpu.VMEM((members, columns), BF16)),
        in_specs=[pl.BlockSpec(memory_space=pltpu.HBM)] * 7,
        out_specs=[pl.BlockSpec(memory_space=pltpu.VMEM)] * 2,
        scratch_shapes=[
            pltpu.SemaphoreType.DMA((1,)),
            pltpu.VMEM((1, own), BF16),
            pltpu.VMEM((1, own), BF16),
            pltpu.VMEM((1, own), jnp.int32),
            pltpu.VMEM((1, own), jnp.int32),
            pltpu.SMEM((1, 1), jnp.int32),
            pltpu.SemaphoreType.DMA((6,)),
            pltpu.VMEM((rows, own), BF16),
            pltpu.VMEM((tiles, rows, slots), BF16),
            pltpu.VMEM((tiles, rows, slots), BF16),
            pltpu.VMEM((points + 2 * half, members, rows), F32),
            pltpu.VMEM(side, F32),
            pltpu.VMEM(side, F32),
            pltpu.VMEM(side, F32),
            pltpu.VMEM(side, F32),
            pltpu.VMEM((count, members, pair), F32),
            pltpu.VMEM((max(lags - 1, 1), count, members, pair), F32),
            pltpu.SemaphoreType.DMA((tiles,)),
            pltpu.SemaphoreType.DMA((tiles,)),
            pltpu.SemaphoreType.DMA((2,)),
            pltpu.SemaphoreType.DMA((2,)),
            pltpu.SemaphoreType.DMA((max(lags - 1, 1),)),
            pltpu.SemaphoreType.DMA((max(lags - 1, 1),)),
            pltpu.VMEM((count, members, pair), F32),
            pltpu.VMEM((rows, slots), BF16),
            pltpu.VMEM((tiles, rows, slots), BF16),
            pltpu.VMEM((half + 1, members, rows), F32),
            pltpu.SemaphoreType.DMA((1,)),
            pltpu.SemaphoreType.DMA((tiles,)),
        ],
        compiler_params=pltpu.CompilerParams(
            collective_id=0, has_side_effects=True, vmem_limit_bytes=LIMIT
        ),
        name="ensemble_weights",
    )(*(
        x if x.size == 1 else pltpu.with_memory_space_constraint(x, pltpu.HBM)
        for x in (
            obs_pert[0], obs_innov, obs_rinv, obs_tile[:, :, 0], obs_column, obs_count, ensemble[0]
        )
    ))
    analysis = pl.pallas_call(
        apply_kernel,
        out_shape=jax.ShapeDtypeStruct((members, columns), BF16),
        in_specs=[pl.BlockSpec(memory_space=pltpu.VMEM)] * 2,
        out_specs=pl.BlockSpec(memory_space=pltpu.HBM),
        scratch_shapes=[
            pltpu.VMEM((members, columns), BF16),
            pltpu.SemaphoreType.DMA(((points + 1) // 3,)),
        ],
        compiler_params=pltpu.CompilerParams(vmem_limit_bytes=LIMIT),
        name="apply_weights",
    )(turned, held)
    return analysis[None]


def solution(mesh):
    return jax.shard_map(
        per_device,
        mesh=mesh,
        in_specs=(
            P("lag", None, "space"),
            P("lag", None, "space"),
            P("lag", "space"),
            P("lag", "space"),
            P("lag", "space", None),
            P("lag", "space"),
            P("lag", "space"),
        ),
        out_specs=P("lag", None, "space"),
        check_vma=False,
    )
```

```python
import functools
import math

import jax
import jax.numpy as jnp
from jax import lax
from jax.experimental import pallas as pl
from jax.experimental.pallas import tpu as pltpu
from jax.sharding import PartitionSpec as P

SPACING = 512
NS_ITERS = 6
BATCHES = [2, 2]
BLOCKS = 4
LIMIT = 24 * 1024 * 1024
LANES = 128
META = 16
BASE = 64
F32 = jnp.float32
BF16 = jnp.bfloat16
NT = (((1,), (1,)), ((), ()))


def halves(x):
    hi = x.astype(BF16)
    return hi, (x - hi.astype(F32)).astype(BF16)


def stationary(hi, lo):
    row = jnp.concatenate([hi, lo], axis=1)
    return jnp.concatenate([row, row], axis=0)


def times(left, weights):
    width = weights.shape[1] // 2
    hi, lo = halves(left)
    out = jnp.dot(jnp.concatenate([hi, lo], axis=1), weights, preferred_element_type=F32)
    return out[:, :width] + out[:, width:]


def partner(me, step, tiles):
    if tiles & (tiles - 1):
        return lax.rem(me + tiles - step, tiles)
    other, bit = me, 1
    while bit < tiles:
        if step & bit:
            other = other + bit - 2 * bit * lax.rem(lax.div(me, bit), 2)
        bit *= 2
    return other


def weights_kernel(
    tiles, lags, slots, group, columns,
    pert_hbm, innov_hbm, rinv_hbm, tile_hbm, col_hbm, count_hbm, ens_hbm,
    turned, ens,
    move_sem,
    innov_ref, rinv_ref, tile_ref, col_ref, count_ref, load_sem,
    msg, snd, rcv, acc, to_left, to_right, from_left, from_right, mine, theirs,
    a2a_send, a2a_recv, halo_send, halo_recv, lag_send, lag_recv, product, edge, edge_rcv, edge_acc, edge_send, edge_recv, ready,
):
    members, own = pert_hbm.shape
    points = columns // SPACING
    half = points // 2
    radius = columns // 2
    pair = 2 * members
    sent = members + META // 2
    me = lax.axis_index("space")
    my_lag = lax.axis_index("lag")

    barrier = pltpu.get_barrier_semaphore()
    blocks_of = BLOCKS if tiles % BLOCKS == 0 else 1
    wide = tiles // blocks_of
    mine_block, inner = lax.div(me, wide), lax.rem(me, wide)

    def rank_of(tile):
        block, place = lax.div(tile, wide), lax.rem(tile, wide)
        digits, bit = block, 1
        while bit < wide:
            digits = digits + lax.rem(lax.div(place, bit), 2)
            bit *= 2
        return digits * tiles + tile

    def before(a, b):
        return lax.div(b - a + span - 1, span)

    span = tiles * (tiles + blocks_of)
    my_rank = rank_of(me)
    ranks_of = [rank_of(jnp.int32(tile)) for tile in range(tiles)]
    earlier = sum(before(r, my_rank) for r in ranks_of)
    for peer in range(tiles - 1, -1, -1):
        @pl.when(my_rank < ranks_of[peer])
        def _(peer=peer):
            pl.semaphore_signal(barrier, inc=1, device_id={"space": peer})
    for step in range(1, lags):
        pl.semaphore_signal(barrier, inc=1, device_id={"lag": lax.rem(my_lag + step, lags)})

    loads = [
        pltpu.make_async_copy(source, dest, load_sem.at[n])
        for n, (source, dest) in enumerate((
            (tile_hbm, tile_ref),
            (count_hbm, count_ref),
            (rinv_hbm, rinv_ref),
            (innov_hbm, innov_ref),
            (col_hbm, col_ref),
            (pert_hbm, msg.at[0:members]),
        ))
    ]
    for load in loads:
        load.start()
    for load in loads:
        load.wait()

    slot_id = lax.broadcasted_iota(jnp.int32, (1, own), 1)
    weight = jnp.where(slot_id < count_ref[0, 0], rinv_ref[...].astype(F32), 0.0)
    column = col_ref[...]
    col_hi = (column // BASE).astype(F32)
    col_lo = (column % BASE).astype(F32)
    row = lax.broadcasted_iota(jnp.int32, (META, own), 0)
    meta = jnp.where(row == 0, weight, 0.0)
    meta = jnp.where(row == 1, innov_ref[...].astype(F32), meta)
    meta = jnp.where(row == 2, col_hi, meta)
    meta = jnp.where(row == 3, col_lo, meta)
    msg[members:, :] = meta.astype(BF16)

    target = tile_ref[...]
    hits = jnp.where(target == lax.broadcasted_iota(jnp.int32, (tiles, own), 0), 1.0, 0.0)
    tri = jnp.where(
        lax.broadcasted_iota(jnp.int32, (LANES, LANES), 0)
        < lax.broadcasted_iota(jnp.int32, (LANES, LANES), 1),
        1.0, 0.0,
    ).astype(BF16)
    seen = jnp.zeros((tiles, 1), F32)
    ranks = []
    for b in range(own // LANES):
        block = hits[:, b * LANES : (b + 1) * LANES]
        ahead = jnp.dot(block.astype(BF16), tri, preferred_element_type=F32) + seen
        ranks.append(jnp.sum(ahead * block, axis=0, keepdims=True))
        seen = seen + jnp.sum(block, axis=1, keepdims=True)
    rank = jnp.concatenate(ranks, axis=1)
    place = lax.broadcasted_iota(jnp.int32, (slots, own), 0).astype(F32).astype(BF16)
    message = msg[...]

    def bucket(dest):
        wanted = jnp.where(target == dest, rank, -1.0).astype(BF16)
        chosen = jnp.where(place == wanted, jnp.ones((), BF16), jnp.zeros((), BF16))
        return lax.dot_general(message, chosen, NT, preferred_element_type=F32).astype(BF16)

    def a2a(step, peer=None):
        return pltpu.make_async_remote_copy(
            src_ref=snd.at[step, 0:sent], dst_ref=rcv.at[step, 0:sent],
            send_sem=a2a_send.at[step], recv_sem=a2a_recv.at[step],
            device_id={"space": me if peer is None else peer},
        )

    pl.semaphore_wait(barrier, earlier + lags - 1)
    for peer in range(tiles):
        @pl.when(ranks_of[peer] < my_rank)
        def _(peer=peer):
            pl.semaphore_signal(ready.at[me], inc=1, device_id={"space": peer})

    def edge_copy(source):
        return pltpu.make_async_remote_copy(
            src_ref=edge.at[0:sent], dst_ref=edge_rcv.at[source, 0:sent],
            send_sem=edge_send.at[0], recv_sem=edge_recv.at[source],
            device_id={"space": 0 * me},
        )

    def step_of(peer):
        block, place = peer // wide, peer % wide
        ahead = lax.rem(mine_block + blocks_of - block, blocks_of)
        return ahead * wide + partner(inner, place, wide)

    def send(peer):
        @pl.when(my_rank < ranks_of[peer])
        def _():
            pl.semaphore_wait(ready.at[peer], 1)

        @pl.when(me != peer)
        def _():
            a2a(step_of(peer), jnp.int32(peer)).start()

    done = 0
    for size in BATCHES + [4] * tiles:
        batch = range(done, min(done + size, tiles))
        for peer in batch:
            snd[step_of(peer)] = bucket(peer)
        if done == 0:
            edge[...] = bucket(tiles - 1)
        for peer in batch:
            send(peer)
        if done == 0:
            @pl.when(me > 0)
            def _():
                edge_copy(me).start()
        done += size
    for step in range(1, tiles):
        rcv[step, sent:] = jnp.zeros((members + META - sent, slots), BF16)

    ens_load = pltpu.make_async_copy(ens_hbm, ens, move_sem.at[0])
    ens_load.start()
    arrivals = list(range(tiles))

    def partials(obs, ks, into, base, fresh):
        pert = obs[0:members].astype(F32)
        info = obs[members:].astype(F32)
        obs_weight = info[0:1]
        places = info[2:3] * BASE + info[3:4]
        for k in ks:
            center = float((k - half) * SPACING + SPACING // 2)
            taper = jnp.maximum(1.0 - jnp.abs(places - center) / radius, 0.0)
            rho = taper * taper * obs_weight
            scaled = (pert * rho).astype(BF16)
            part = lax.dot_general(scaled, obs, NT, preferred_element_type=F32)
            if fresh:
                into[k - base] = part
            else:
                into[k - base] += part

    for first in range(0, tiles, group):
        for step in arrivals[max(first, 1) : first + group]:
            a2a(step).wait_recv()
        obs = jnp.concatenate(
            [rcv[step] if step else snd[0] for step in arrivals[first : first + group]], axis=1
        )

        def moments(ks, obs=obs, first=first):
            partials(obs, ks, acc, 0, first == 0)

        @pl.when(me == 0)
        def _(first=first):
            for step in arrivals[max(first, 1) : first + group]:
                edge_copy(step).wait_recv()
            near = [
                edge_rcv[step] if step else edge[...] for step in arrivals[first : first + group]
            ]
            partials(
                jnp.concatenate(near, axis=1), range(points + half - 1, points + 2 * half),
                edge_acc, points + half - 1, first == 0,
            )

        if first + group < tiles:
            moments(range(points + 2 * half))

    lane = lax.broadcasted_iota(jnp.int32, (members, pair), 1)
    low = lane < members

    def joined(a, b, source=acc):
        return jnp.concatenate([source[a, :, 0:members], source[b, :, 0:members]], axis=1)

    def drive_of(a, source=acc):
        return source[a, :, members + 1 : members + 2]

    left_copy = pltpu.make_async_remote_copy(
        src_ref=to_left, dst_ref=from_right, send_sem=halo_send.at[0], recv_sem=halo_recv.at[0],
        device_id={"space": lax.rem(me + tiles - 1, tiles)},
    )
    right_copy = pltpu.make_async_remote_copy(
        src_ref=to_right, dst_ref=from_left, send_sem=halo_send.at[1], recv_sem=halo_recv.at[1],
        device_id={"space": lax.rem(me + 1, tiles)},
    )

    fold = members // 2
    row = lax.broadcasted_iota(jnp.int32, (members, pair), 0)
    within = lax.rem(lane, members)
    strip = lax.broadcasted_iota(jnp.int32, (fold, pair), 1) - members

    def packed(single, ks, source=acc):
        first = [joined(ks[n], ks[n + 1], source) for n in range(0, half, 2)]
        columns = [drive_of(k, source) for k in sorted([single, *ks])]
        for other in first[1::2]:
            diag = jnp.where(row == within, other, 0.0)
            columns.append(jnp.sum(jnp.where(low, diag, 0.0), axis=1, keepdims=True))
            columns.append(jnp.sum(jnp.where(low, 0.0, diag), axis=1, keepdims=True))
        parts = [
            jnp.where(row <= within, first[n], first[n + 1]) for n in range(0, half // 2, 2)
        ]
        tail = jnp.concatenate(
            [source[single, 0:fold, 0:members], source[single, fold:members, 0:members]], axis=1
        )
        for n, column in enumerate(columns):
            tail = jnp.where(strip == 2 * n, column[0:fold], tail)
            tail = jnp.where(strip == 2 * n + 1, column[fold:], tail)
        return jnp.concatenate([*parts, tail], axis=0)

    def unpacked(ref):
        tail = ref[members * (half // 4) :]

        def column(n):
            return jnp.concatenate(
                [
                    tail[:, members + 2 * n : members + 2 * n + 1],
                    tail[:, members + 2 * n + 1 : members + 2 * n + 2],
                ],
                axis=0,
            )

        pairs = []
        for n in range(half // 4):
            part = ref[n * members : (n + 1) * members]
            turned_part = jnp.concatenate([part[:, 0:members].T, part[:, members:].T], axis=1)
            pairs.append(jnp.where(row <= within, part, turned_part))
            diag = jnp.where(low, column(half + 1 + 2 * n), column(half + 2 + 2 * n))
            other = jnp.where(row == within, diag, turned_part)
            pairs.append(jnp.where(row > within, part, other))
        corner = tail[:, 0:members].T[fold:]
        bottom = jnp.concatenate([corner, tail[:, members + fold :]], axis=1)
        single = jnp.concatenate([tail[:, 0:members], bottom], axis=0)
        return pairs, single, [column(n) for n in range(half + 1)]

    last = points + 2 * half - 1
    moments(range(half + 1))
    to_left[...] = packed(0, list(range(1, half + 1)))
    moments(range(last - half, last + 1))
    left_copy.start()
    to_right[...] = packed(last, list(range(last - half, last)))

    moments(range(half + 1, half + 3))

    @pl.when(me < tiles - 1)
    def _():
        right_copy.start()

    moments(range(half + 3, last - half))

    eye = jnp.where(
        lax.rem(lane, members) == lax.broadcasted_iota(jnp.int32, (members, pair), 0), 1.0, 0.0
    )
    mask_low = jnp.where(low, 1.0, 0.0).astype(BF16)
    mask_high = jnp.where(low, 0.0, 1.0).astype(BF16)

    def diagonal(x):
        return jnp.concatenate([x * mask_low, x * mask_high], axis=0)

    def blocks(x):
        hi, lo = halves(x)
        return stationary(diagonal(hi), diagonal(lo))


    count = (points + 2) // 2
    own_pairs = [joined(half - 1 + 2 * i, half + 2 * i) for i in range(count)]
    own_drives = [drive_of(half - 1 + j) for j in range(points + 2)]
    left_copy.wait_recv()

    @pl.when(me > 0)
    def _():
        right_copy.wait_recv()

    @pl.when(me == 0)
    def _():
        from_left[...] = packed(half, list(range(half)), edge_acc)

    lefts, left_single, left_drives = unpacked(from_left)
    rights, right_single, right_drives = unpacked(from_right)

    grams = []
    for i in range(count):
        total = own_pairs[i] + (members - 1.0) * eye
        if i < half // 2:
            total = total + lefts[i]
        elif i == half // 2:
            total = total + jnp.concatenate([left_single, right_single], axis=1)
        else:
            total = total + rights[i - half // 2 - 1]
        grams.append(total)
    drives = [
        own + other for own, other in zip(own_drives, [*left_drives, *right_drives])
    ]

    uppers, lowers, scales = [], [], []
    for total in grams:
        squares = jnp.sum(total * total, axis=0, keepdims=True)
        row_low = lax.broadcasted_iota(jnp.int32, (1, pair), 1) < members
        sum_low = jnp.sum(jnp.where(row_low, squares, 0.0), axis=1, keepdims=True)
        sum_high = jnp.sum(jnp.where(row_low, 0.0, squares), axis=1, keepdims=True)
        scale = jnp.sqrt(jnp.where(row_low, sum_low, sum_high))
        scales.append(scale)
        uppers.append(total / scale)

    for sweep in range(NS_ITERS):
        if sweep == 0:
            middles = [1.5 * eye - 0.5 * up for up in uppers]
            lowers = middles
            uppers = [times(up, blocks(mid)) for up, mid in zip(uppers, middles)]
        else:
            middles = [
                1.5 * eye - 0.5 * times(lo, blocks(up)) for lo, up in zip(lowers, uppers)
            ]
            if sweep < NS_ITERS - 1:
                both = [
                    times(jnp.concatenate([up, lo], axis=0), blocks(mid))
                    for up, lo, mid in zip(uppers, lowers, middles)
                ]
                uppers = [x[0:members] for x in both]
                lowers = [x[members:] for x in both]
            else:
                lowers = [times(lo, blocks(mid)) for lo, mid in zip(lowers, middles)]

    results = []
    for i in range(count):
        root = lowers[i] / jnp.sqrt(scales[i])
        top = jnp.where(low, drives[2 * i], 0.0)
        bottom = jnp.where(low, 0.0, drives[2 * i + 1])
        hi, lo = halves(jnp.concatenate([top, bottom], axis=0))
        inner = times(root, stationary(hi, lo))
        shift = times(root, blocks(inner))
        full = math.sqrt(members - 1.0) * root + shift
        results.append(full - jnp.mean(full, axis=0, keepdims=True) + 1.0 / members)
    for i in range(count):
        mine[i] = results[i]
        product[i] = results[i]

    def lag_copy(step):
        return pltpu.make_async_remote_copy(
            src_ref=mine, dst_ref=theirs.at[step - 1],
            send_sem=lag_send.at[step - 1], recv_sem=lag_recv.at[step - 1],
            device_id={"lag": lax.rem(my_lag + lags - step, lags)},
        )

    for step in range(1, lags):
        @pl.when(my_lag >= step)
        def _(step=step):
            lag_copy(step).start()
    for step in range(1, lags):
        @pl.when(my_lag + step < lags)
        def _(step=step):
            lag_copy(step).wait_recv()
            for i in range(count):
                product[i] = times(product[i], blocks(theirs[step - 1, i]))
    for i in range(count):
        turned[i * pair : (i + 1) * pair] = product[i].T.astype(BF16)
    ens_load.wait()

    for step in range(1, tiles):
        a2a(step).wait_send()
    left_copy.wait_send()

    @pl.when(me < tiles - 1)
    def _():
        right_copy.wait_send()

    @pl.when(me > 0)
    def _():
        edge_copy(me).wait_send()

    for step in range(1, lags):
        @pl.when(my_lag >= step)
        def _(step=step):
            lag_copy(step).wait_send()


def apply_kernel(turned, ens, out_hbm, out, store_sem):
    members, columns = ens.shape
    points = columns // SPACING
    stores = []
    half_span = SPACING // 2
    for s in range(points + 1):
        start = max(s * SPACING - half_span, 0)
        stop = min(s * SPACING + half_span, columns)
        both = jnp.dot(
            turned[s * members : (s + 2) * members], ens[:, start:stop],
            preferred_element_type=F32,
        )
        along = lax.broadcasted_iota(jnp.int32, (1, stop - start), 1).astype(F32)
        second = (along + float(start - (s * SPACING - half_span))) / SPACING
        mixed = both[0:members] * (1.0 - second) + both[members:] * second
        out[:, start:stop] = mixed.astype(BF16)
        if s % 3 == 2:
            first = max((s - 2) * SPACING - half_span, 0)
            store = pltpu.make_async_copy(
                out.at[:, first:stop], out_hbm.at[:, first:stop], store_sem.at[s // 3]
            )
            store.start()
            stores.append(store)
    for store in stores:
        store.wait()


def per_device(ensemble, obs_pert, obs_innov, obs_rinv, obs_tile, obs_column, obs_count):
    members, columns = ensemble.shape[1:]
    own = obs_pert.shape[2]
    tiles, lags = lax.axis_size("space"), lax.axis_size("lag")
    slot_size = max(2, 2 * own // tiles)
    slots = -(-slot_size // LANES) * LANES
    group = 4
    points = columns // SPACING
    half = points // 2
    count = (points + 2) // 2
    pair = 2 * members
    rows = members + META
    side = (members * (half // 4) + members // 2, pair)
    turned, held = pl.pallas_call(
        functools.partial(weights_kernel, tiles, lags, slots, group, columns),
        out_shape=(pltpu.VMEM((count * pair, members), BF16), pltpu.VMEM((members, columns), BF16)),
        in_specs=[pl.BlockSpec(memory_space=pltpu.HBM)] * 7,
        out_specs=[pl.BlockSpec(memory_space=pltpu.VMEM)] * 2,
        scratch_shapes=[
            pltpu.SemaphoreType.DMA((1,)),
            pltpu.VMEM((1, own), BF16),
            pltpu.VMEM((1, own), BF16),
            pltpu.VMEM((1, own), jnp.int32),
            pltpu.VMEM((1, own), jnp.int32),
            pltpu.SMEM((1, 1), jnp.int32),
            pltpu.SemaphoreType.DMA((6,)),
            pltpu.VMEM((rows, own), BF16),
            pltpu.VMEM((tiles, rows, slots), BF16),
            pltpu.VMEM((tiles, rows, slots), BF16),
            pltpu.VMEM((points + 2 * half, members, rows), F32),
            pltpu.VMEM(side, F32),
            pltpu.VMEM(side, F32),
            pltpu.VMEM(side, F32),
            pltpu.VMEM(side, F32),
            pltpu.VMEM((count, members, pair), F32),
            pltpu.VMEM((max(lags - 1, 1), count, members, pair), F32),
            pltpu.SemaphoreType.DMA((tiles,)),
            pltpu.SemaphoreType.DMA((tiles,)),
            pltpu.SemaphoreType.DMA((2,)),
            pltpu.SemaphoreType.DMA((2,)),
            pltpu.SemaphoreType.DMA((max(lags - 1, 1),)),
            pltpu.SemaphoreType.DMA((max(lags - 1, 1),)),
            pltpu.VMEM((count, members, pair), F32),
            pltpu.VMEM((rows, slots), BF16),
            pltpu.VMEM((tiles, rows, slots), BF16),
            pltpu.VMEM((half + 1, members, rows), F32),
            pltpu.SemaphoreType.DMA((1,)),
            pltpu.SemaphoreType.DMA((tiles,)),
            pltpu.SemaphoreType.REGULAR((tiles,)),
        ],
        compiler_params=pltpu.CompilerParams(
            collective_id=0, has_side_effects=True, vmem_limit_bytes=LIMIT
        ),
        name="ensemble_weights",
    )(*(
        x if x.size == 1 else pltpu.with_memory_space_constraint(x, pltpu.HBM)
        for x in (
            obs_pert[0], obs_innov, obs_rinv, obs_tile[:, :, 0], obs_column, obs_count, ensemble[0]
        )
    ))
    analysis = pl.pallas_call(
        apply_kernel,
        out_shape=jax.ShapeDtypeStruct((members, columns), BF16),
        in_specs=[pl.BlockSpec(memory_space=pltpu.VMEM)] * 2,
        out_specs=pl.BlockSpec(memory_space=pltpu.HBM),
        scratch_shapes=[
            pltpu.VMEM((members, columns), BF16),
            pltpu.SemaphoreType.DMA(((points + 1) // 3,)),
        ],
        compiler_params=pltpu.CompilerParams(vmem_limit_bytes=LIMIT),
        name="apply_weights",
    )(turned, held)
    return analysis[None]


def solution(mesh):
    return jax.shard_map(
        per_device,
        mesh=mesh,
        in_specs=(
            P("lag", None, "space"),
            P("lag", None, "space"),
            P("lag", "space"),
            P("lag", "space"),
            P("lag", "space", None),
            P("lag", "space"),
            P("lag", "space"),
        ),
        out_specs=P("lag", None, "space"),
        check_vma=False,
    )
```

```python
import functools
import math

import jax
import jax.numpy as jnp
from jax import lax
from jax.experimental import pallas as pl
from jax.experimental.pallas import tpu as pltpu
from jax.sharding import PartitionSpec as P

SPACING = 512
NS_ITERS = 6
THIN = 16
BATCHES = [2, 2]
BLOCKS = 4
LIMIT = 24 * 1024 * 1024
LANES = 128
META = 16
BASE = 64
F32 = jnp.float32
BF16 = jnp.bfloat16
NT = (((1,), (1,)), ((), ()))


def halves(x):
    hi = x.astype(BF16)
    return hi, (x - hi.astype(F32)).astype(BF16)


def stationary(hi, lo):
    row = jnp.concatenate([hi, lo], axis=1)
    return jnp.concatenate([row, row], axis=0)


def times(left, weights):
    width = weights.shape[1] // 2
    hi, lo = halves(left)
    out = jnp.dot(jnp.concatenate([hi, lo], axis=1), weights, preferred_element_type=F32)
    return out[:, :width] + out[:, width:]


def partner(me, step, tiles):
    if tiles & (tiles - 1):
        return lax.rem(me + tiles - step, tiles)
    other, bit = me, 1
    while bit < tiles:
        if step & bit:
            other = other + bit - 2 * bit * lax.rem(lax.div(me, bit), 2)
        bit *= 2
    return other


def weights_kernel(
    tiles, lags, slots, group, columns,
    pert_hbm, innov_hbm, rinv_hbm, tile_hbm, col_hbm, count_hbm, ens_hbm,
    turned, ens,
    move_sem,
    innov_ref, rinv_ref, tile_ref, col_ref, count_ref, load_sem,
    msg, snd, rcv, acc, to_left, to_right, from_left, from_right, mine, theirs,
    a2a_send, a2a_recv, halo_send, halo_recv, lag_send, lag_recv, product, edge, edge_rcv, edge_acc, edge_send, edge_recv, ready,
):
    members, own = pert_hbm.shape
    points = columns // SPACING
    half = points // 2
    radius = columns // 2
    pair = 2 * members
    sent = members + META // 2
    me = lax.axis_index("space")
    my_lag = lax.axis_index("lag")

    barrier = pltpu.get_barrier_semaphore()
    blocks_of = BLOCKS if tiles % BLOCKS == 0 else 1
    wide = tiles // blocks_of
    mine_block, inner = lax.div(me, wide), lax.rem(me, wide)

    def rank_of(tile):
        block, place = lax.div(tile, wide), lax.rem(tile, wide)
        digits, bit = block, 1
        while bit < wide:
            digits = digits + lax.rem(lax.div(place, bit), 2)
            bit *= 2
        return digits * tiles + tile

    def before(a, b):
        return lax.div(b - a + span - 1, span)

    span = tiles * (tiles + blocks_of)
    my_rank = rank_of(me)
    ranks_of = [rank_of(jnp.int32(tile)) for tile in range(tiles)]
    earlier = sum(before(r, my_rank) for r in ranks_of)
    for peer in range(tiles - 1, -1, -1):
        @pl.when(my_rank < ranks_of[peer])
        def _(peer=peer):
            pl.semaphore_signal(barrier, inc=1, device_id={"space": peer})
    for step in range(1, lags):
        pl.semaphore_signal(barrier, inc=1, device_id={"lag": lax.rem(my_lag + step, lags)})

    loads = [
        pltpu.make_async_copy(source, dest, load_sem.at[n])
        for n, (source, dest) in enumerate((
            (tile_hbm, tile_ref),
            (count_hbm, count_ref),
            (rinv_hbm, rinv_ref),
            (innov_hbm, innov_ref),
            (col_hbm, col_ref),
            (pert_hbm, msg.at[0:members]),
        ))
    ]
    for load in loads:
        load.start()
    for load in loads:
        load.wait()

    slot_id = lax.broadcasted_iota(jnp.int32, (1, own), 1)
    weight = jnp.where(slot_id < count_ref[0, 0], rinv_ref[...].astype(F32), 0.0)
    column = col_ref[...]
    col_hi = (column // BASE).astype(F32)
    col_lo = (column % BASE).astype(F32)
    row = lax.broadcasted_iota(jnp.int32, (META, own), 0)
    meta = jnp.where(row == 0, weight, 0.0)
    meta = jnp.where(row == 1, innov_ref[...].astype(F32), meta)
    meta = jnp.where(row == 2, col_hi, meta)
    meta = jnp.where(row == 3, col_lo, meta)
    msg[members:, :] = meta.astype(BF16)

    target = tile_ref[...]
    hits = jnp.where(target == lax.broadcasted_iota(jnp.int32, (tiles, own), 0), 1.0, 0.0)
    tri = jnp.where(
        lax.broadcasted_iota(jnp.int32, (LANES, LANES), 0)
        < lax.broadcasted_iota(jnp.int32, (LANES, LANES), 1),
        1.0, 0.0,
    ).astype(BF16)
    seen = jnp.zeros((tiles, 1), F32)
    ranks = []
    for b in range(own // LANES):
        block = hits[:, b * LANES : (b + 1) * LANES]
        ahead = jnp.dot(block.astype(BF16), tri, preferred_element_type=F32) + seen
        ranks.append(jnp.sum(ahead * block, axis=0, keepdims=True))
        seen = seen + jnp.sum(block, axis=1, keepdims=True)
    rank = jnp.concatenate(ranks, axis=1)
    place = lax.broadcasted_iota(jnp.int32, (slots, own), 0).astype(F32).astype(BF16)
    message = msg[...]

    def bucket(dest):
        wanted = jnp.where(target == dest, rank, -1.0).astype(BF16)
        chosen = jnp.where(place == wanted, jnp.ones((), BF16), jnp.zeros((), BF16))
        return lax.dot_general(message, chosen, NT, preferred_element_type=F32).astype(BF16)

    def a2a(step, peer=None):
        return pltpu.make_async_remote_copy(
            src_ref=snd.at[step, 0:sent], dst_ref=rcv.at[step, 0:sent],
            send_sem=a2a_send.at[step], recv_sem=a2a_recv.at[step],
            device_id={"space": me if peer is None else peer},
        )

    pl.semaphore_wait(barrier, earlier + lags - 1)
    for peer in range(tiles):
        @pl.when(ranks_of[peer] < my_rank)
        def _(peer=peer):
            pl.semaphore_signal(ready.at[me], inc=1, device_id={"space": peer})

    def edge_copy(source):
        return pltpu.make_async_remote_copy(
            src_ref=edge.at[0:sent], dst_ref=edge_rcv.at[source, 0:sent],
            send_sem=edge_send.at[0], recv_sem=edge_recv.at[source],
            device_id={"space": 0 * me},
        )

    def step_of(peer):
        block, place = peer // wide, peer % wide
        ahead = lax.rem(mine_block + blocks_of - block, blocks_of)
        return ahead * wide + partner(inner, place, wide)

    def send(peer):
        @pl.when(my_rank < ranks_of[peer])
        def _():
            pl.semaphore_wait(ready.at[peer], 1)

        @pl.when(me != peer)
        def _():
            a2a(step_of(peer), jnp.int32(peer)).start()

    done = 0
    for size in BATCHES + [4] * tiles:
        batch = range(done, min(done + size, tiles))
        for peer in batch:
            snd[step_of(peer)] = bucket(peer)
        if done == 0:
            edge[...] = bucket(tiles - 1)
        for peer in batch:
            send(peer)
        if done == 0:
            @pl.when(me > 0)
            def _():
                edge_copy(me).start()
        done += size
    for step in range(1, tiles):
        rcv[step, sent:] = jnp.zeros((members + META - sent, slots), BF16)

    ens_load = pltpu.make_async_copy(ens_hbm, ens, move_sem.at[0])
    ens_load.start()
    arrivals = list(range(tiles))

    def partials(obs, ks, into, base, fresh):
        pert = obs[0:members].astype(F32)
        info = obs[members:].astype(F32)
        obs_weight = info[0:1]
        places = info[2:3] * BASE + info[3:4]
        for k in ks:
            center = float((k - half) * SPACING + SPACING // 2)
            taper = jnp.maximum(1.0 - jnp.abs(places - center) / radius, 0.0)
            rho = taper * taper * obs_weight
            scaled = (pert * rho).astype(BF16)
            part = lax.dot_general(obs, scaled, NT, preferred_element_type=F32)
            if fresh:
                into[k - base] = part
            else:
                into[k - base] += part

    for first in range(0, tiles, group):
        for step in arrivals[max(first, 1) : first + group]:
            a2a(step).wait_recv()
        obs = jnp.concatenate(
            [rcv[step] if step else snd[0] for step in arrivals[first : first + group]], axis=1
        )

        def moments(ks, obs=obs, first=first):
            partials(obs, ks, acc, 0, first == 0)

        @pl.when(me == 0)
        def _(first=first):
            for step in arrivals[max(first, 1) : first + group]:
                edge_copy(step).wait_recv()
            near = [
                edge_rcv[step] if step else edge[...] for step in arrivals[first : first + group]
            ]
            partials(
                jnp.concatenate(near, axis=1), range(points + half - 1, points + 2 * half),
                edge_acc, points + half - 1, first == 0,
            )

        if first + group < tiles:
            moments(range(points + 2 * half))

    lane = lax.broadcasted_iota(jnp.int32, (members, pair), 1)
    low = lane < members

    def joined(a, b, source=acc):
        return jnp.concatenate([source[a, 0:members], source[b, 0:members]], axis=1)

    def drives_of(a, b, source=acc):
        none = jnp.zeros((1, members), F32)
        return jnp.concatenate(
            [none if k is None else source[k, members + 1 : members + 2] for k in (a, b)], axis=1
        )

    left_copy = pltpu.make_async_remote_copy(
        src_ref=to_left, dst_ref=from_right, send_sem=halo_send.at[0], recv_sem=halo_recv.at[0],
        device_id={"space": lax.rem(me + tiles - 1, tiles)},
    )
    right_copy = pltpu.make_async_remote_copy(
        src_ref=to_right, dst_ref=from_left, send_sem=halo_send.at[1], recv_sem=halo_recv.at[1],
        device_id={"space": lax.rem(me + 1, tiles)},
    )

    fold = members // 2
    extra = members * (half // 4) + fold
    row = lax.broadcasted_iota(jnp.int32, (members, pair), 0)
    within = lax.rem(lane, members)

    def packed(single, ks, source=acc):
        first = [joined(ks[n], ks[n + 1], source) for n in range(0, half, 2)]
        ends = (None, single) if single < ks[0] else (single, None)
        vectors = [drives_of(ks[n], ks[n + 1], source) for n in range(0, half, 2)]
        vectors.append(drives_of(*ends, source))
        vectors += [
            jnp.sum(jnp.where(row == within, other, 0.0), axis=0, keepdims=True)
            for other in first[1::2]
        ]
        spare = -len(vectors) % 8
        if spare:
            vectors.append(jnp.zeros((spare, pair), F32))
        parts = [
            jnp.where(row <= within, first[n], first[n + 1]) for n in range(0, half // 2, 2)
        ]
        tail = jnp.concatenate(
            [source[single, 0:fold], source[single, fold:members]], axis=1
        )
        return jnp.concatenate([*parts, tail, *vectors], axis=0)

    def unpacked(ref):
        pairs = []
        for n in range(half // 4):
            part = ref[n * members : (n + 1) * members]
            flipped = jnp.concatenate([part[:, 0:members].T, part[:, members:].T], axis=1)
            pairs.append(jnp.where(row <= within, part, flipped))
            at = extra + half // 2 + 1 + n
            other = jnp.where(row == within, ref[at : at + 1], flipped)
            pairs.append(jnp.where(row > within, part, other))
        tail = ref[extra - fold : extra]
        corner = tail[:, 0:members].T[fold:]
        bottom = jnp.concatenate([corner, tail[:, members + fold :]], axis=1)
        single = jnp.concatenate([tail[:, 0:members], bottom], axis=0)
        return pairs, single, [ref[extra + n : extra + n + 1] for n in range(half // 2 + 1)]

    last = points + 2 * half - 1
    moments(range(half + 1))
    to_left[...] = packed(0, list(range(1, half + 1)))
    moments(range(last - half, last + 1))
    left_copy.start()
    to_right[...] = packed(last, list(range(last - half, last)))

    moments(range(half + 1, half + 3))

    @pl.when(me < tiles - 1)
    def _():
        right_copy.start()

    moments(range(half + 3, last - half))

    eye = jnp.where(
        lax.rem(lane, members) == lax.broadcasted_iota(jnp.int32, (members, pair), 0), 1.0, 0.0
    )
    mask_low = jnp.where(low, 1.0, 0.0).astype(BF16)
    mask_high = jnp.where(low, 0.0, 1.0).astype(BF16)

    def diagonal(x):
        return jnp.concatenate([x * mask_low, x * mask_high], axis=0)

    def blocks(x):
        hi, lo = halves(x)
        return stationary(diagonal(hi), diagonal(lo))


    count = (points + 2) // 2
    own_pairs = [joined(half - 1 + 2 * i, half + 2 * i) for i in range(count)]
    own_drives = [drives_of(half - 1 + 2 * i, half + 2 * i) for i in range(count)]
    left_copy.wait_recv()

    @pl.when(me > 0)
    def _():
        right_copy.wait_recv()

    @pl.when(me == 0)
    def _():
        from_left[...] = packed(half, list(range(half)), edge_acc)

    lefts, left_single, left_drives = unpacked(from_left)
    rights, right_single, right_drives = unpacked(from_right)

    grams = []
    for i in range(count):
        total = own_pairs[i] + (members - 1.0) * eye
        if i < half // 2:
            total = total + lefts[i]
        elif i == half // 2:
            total = total + jnp.concatenate([left_single, right_single], axis=1)
        else:
            total = total + rights[i - half // 2 - 1]
        grams.append(total)
    drives = [
        own_drives[i]
        + (left_drives[i] if i < half // 2 else 0.0)
        + (right_drives[i - half // 2 - 1] if i > half // 2 else 0.0)
        for i in range(count)
    ]
    drives[half // 2] += left_drives[half // 2] + right_drives[half // 2]

    states, scales = [], []
    row_low = lax.broadcasted_iota(jnp.int32, (1, pair), 1) < members
    for total in grams:
        squares = jnp.sum(total * total, axis=0, keepdims=True)
        sum_low = jnp.sum(jnp.where(row_low, squares, 0.0), axis=1, keepdims=True)
        sum_high = jnp.sum(jnp.where(row_low, 0.0, squares), axis=1, keepdims=True)
        scale = jnp.sqrt(jnp.where(row_low, sum_low, sum_high))
        scales.append(scale)
        states.append(total / scale)
    drives = [jnp.broadcast_to(drive, (THIN, pair)) for drive in drives]

    lowers = []
    for sweep in range(NS_ITERS):
        middles = [1.5 * eye - 0.5 * state for state in states]
        weights = [blocks(mid) for mid in middles]
        final = sweep == NS_ITERS - 1
        lefts = [
            ([] if final else [states[i]]) + ([lowers[i]] if sweep else []) + [drives[i]]
            for i in range(count)
        ]
        once = [times(jnp.concatenate(left, axis=0), w) for left, w in zip(lefts, weights)]
        lowers = [x[-THIN - members : -THIN] for x in once] if sweep else middles
        again = [
            x[-THIN:] if final else jnp.concatenate([x[0:members], x[-THIN:]], axis=0)
            for x in once
        ]
        twice = [times(left, w) for left, w in zip(again, weights)]
        states = [x[0:members] for x in twice]
        drives = [x[-THIN:] for x in twice]

    def centered(x):
        sum_low = jnp.sum(jnp.where(low[0:1], x, 0.0), axis=1, keepdims=True)
        sum_high = jnp.sum(jnp.where(low[0:1], 0.0, x), axis=1, keepdims=True)
        return x - jnp.where(low[0:1], sum_low, sum_high) / members

    results = []
    for i in range(count):
        root = lowers[i] / jnp.sqrt(scales[i])
        shift = drives[i][0:1] / scales[i]
        full = math.sqrt(members - 1.0) * root + shift
        results.append(centered(full) + 1.0 / members)
    for i in range(count):
        mine[i] = results[i]
        product[i] = results[i]

    def lag_copy(step):
        return pltpu.make_async_remote_copy(
            src_ref=mine, dst_ref=theirs.at[step - 1],
            send_sem=lag_send.at[step - 1], recv_sem=lag_recv.at[step - 1],
            device_id={"lag": lax.rem(my_lag + lags - step, lags)},
        )

    for step in range(1, lags):
        @pl.when(my_lag >= step)
        def _(step=step):
            lag_copy(step).start()
    for step in range(1, lags):
        @pl.when(my_lag + step < lags)
        def _(step=step):
            lag_copy(step).wait_recv()
            for i in range(count):
                product[i] = times(theirs[step - 1, i], blocks(product[i]))
    for i in range(count):
        both = product[i].astype(BF16)
        turned[i * pair : i * pair + members] = both[:, 0:members]
        turned[i * pair + members : (i + 1) * pair] = both[:, members:]
    ens_load.wait()

    for step in range(1, tiles):
        a2a(step).wait_send()
    left_copy.wait_send()

    @pl.when(me < tiles - 1)
    def _():
        right_copy.wait_send()

    @pl.when(me > 0)
    def _():
        edge_copy(me).wait_send()

    for step in range(1, lags):
        @pl.when(my_lag >= step)
        def _(step=step):
            lag_copy(step).wait_send()


def apply_kernel(turned, ens, out_hbm, out, store_sem):
    members, columns = ens.shape
    points = columns // SPACING
    stores = []
    half_span = SPACING // 2
    for s in range(points + 1):
        start = max(s * SPACING - half_span, 0)
        stop = min(s * SPACING + half_span, columns)
        both = jnp.dot(
            turned[s * members : (s + 2) * members], ens[:, start:stop],
            preferred_element_type=F32,
        )
        along = lax.broadcasted_iota(jnp.int32, (1, stop - start), 1).astype(F32)
        second = (along + float(start - (s * SPACING - half_span))) / SPACING
        mixed = both[0:members] * (1.0 - second) + both[members:] * second
        out[:, start:stop] = mixed.astype(BF16)
        if s % 3 == 2:
            first = max((s - 2) * SPACING - half_span, 0)
            store = pltpu.make_async_copy(
                out.at[:, first:stop], out_hbm.at[:, first:stop], store_sem.at[s // 3]
            )
            store.start()
            stores.append(store)
    for store in stores:
        store.wait()


def per_device(ensemble, obs_pert, obs_innov, obs_rinv, obs_tile, obs_column, obs_count):
    members, columns = ensemble.shape[1:]
    own = obs_pert.shape[2]
    tiles, lags = lax.axis_size("space"), lax.axis_size("lag")
    slot_size = max(2, 2 * own // tiles)
    slots = -(-slot_size // LANES) * LANES
    group = 4
    points = columns // SPACING
    half = points // 2
    count = (points + 2) // 2
    pair = 2 * members
    rows = members + META
    vectors = half // 2 + 1 + half // 4
    side = (members * (half // 4) + members // 2 + -(-vectors // 8) * 8, pair)
    turned, held = pl.pallas_call(
        functools.partial(weights_kernel, tiles, lags, slots, group, columns),
        out_shape=(pltpu.VMEM((count * pair, members), BF16), pltpu.VMEM((members, columns), BF16)),
        in_specs=[pl.BlockSpec(memory_space=pltpu.HBM)] * 7,
        out_specs=[pl.BlockSpec(memory_space=pltpu.VMEM)] * 2,
        scratch_shapes=[
            pltpu.SemaphoreType.DMA((1,)),
            pltpu.VMEM((1, own), BF16),
            pltpu.VMEM((1, own), BF16),
            pltpu.VMEM((1, own), jnp.int32),
            pltpu.VMEM((1, own), jnp.int32),
            pltpu.SMEM((1, 1), jnp.int32),
            pltpu.SemaphoreType.DMA((6,)),
            pltpu.VMEM((rows, own), BF16),
            pltpu.VMEM((tiles, rows, slots), BF16),
            pltpu.VMEM((tiles, rows, slots), BF16),
            pltpu.VMEM((points + 2 * half, rows, members), F32),
            pltpu.VMEM(side, F32),
            pltpu.VMEM(side, F32),
            pltpu.VMEM(side, F32),
            pltpu.VMEM(side, F32),
            pltpu.VMEM((count, members, pair), F32),
            pltpu.VMEM((max(lags - 1, 1), count, members, pair), F32),
            pltpu.SemaphoreType.DMA((tiles,)),
            pltpu.SemaphoreType.DMA((tiles,)),
            pltpu.SemaphoreType.DMA((2,)),
            pltpu.SemaphoreType.DMA((2,)),
            pltpu.SemaphoreType.DMA((max(lags - 1, 1),)),
            pltpu.SemaphoreType.DMA((max(lags - 1, 1),)),
            pltpu.VMEM((count, members, pair), F32),
            pltpu.VMEM((rows, slots), BF16),
            pltpu.VMEM((tiles, rows, slots), BF16),
            pltpu.VMEM((half + 1, rows, members), F32),
            pltpu.SemaphoreType.DMA((1,)),
            pltpu.SemaphoreType.DMA((tiles,)),
            pltpu.SemaphoreType.REGULAR((tiles,)),
        ],
        compiler_params=pltpu.CompilerParams(
            collective_id=0, has_side_effects=True, vmem_limit_bytes=LIMIT
        ),
        name="ensemble_weights",
    )(*(
        x if x.size == 1 else pltpu.with_memory_space_constraint(x, pltpu.HBM)
        for x in (
            obs_pert[0], obs_innov, obs_rinv, obs_tile[:, :, 0], obs_column, obs_count, ensemble[0]
        )
    ))
    analysis = pl.pallas_call(
        apply_kernel,
        out_shape=jax.ShapeDtypeStruct((members, columns), BF16),
        in_specs=[pl.BlockSpec(memory_space=pltpu.VMEM)] * 2,
        out_specs=pl.BlockSpec(memory_space=pltpu.HBM),
        scratch_shapes=[
            pltpu.VMEM((members, columns), BF16),
            pltpu.SemaphoreType.DMA(((points + 1) // 3,)),
        ],
        compiler_params=pltpu.CompilerParams(vmem_limit_bytes=LIMIT),
        name="apply_weights",
    )(turned, held)
    return analysis[None]


def solution(mesh):
    return jax.shard_map(
        per_device,
        mesh=mesh,
        in_specs=(
            P("lag", None, "space"),
            P("lag", None, "space"),
            P("lag", "space"),
            P("lag", "space"),
            P("lag", "space", None),
            P("lag", "space"),
            P("lag", "space"),
        ),
        out_specs=P("lag", None, "space"),
        check_vma=False,
    )
```

```python
import functools
import math

import jax
import jax.numpy as jnp
from jax import lax
from jax.experimental import pallas as pl
from jax.experimental.pallas import tpu as pltpu
from jax.sharding import PartitionSpec as P

SPACING = 512
NS_ITERS = 6
THIN = 16
BLOCKS = 4
LIMIT = 24 * 1024 * 1024
LANES = 128
META = 16
BASE = 64
F32 = jnp.float32
BF16 = jnp.bfloat16
NT = (((1,), (1,)), ((), ()))


def halves(x):
    hi = x.astype(BF16)
    return hi, (x - hi.astype(F32)).astype(BF16)


def stationary(hi, lo):
    row = jnp.concatenate([hi, lo], axis=1)
    return jnp.concatenate([row, row], axis=0)


def times(left, weights):
    width = weights.shape[1] // 2
    hi, lo = halves(left)
    out = jnp.dot(jnp.concatenate([hi, lo], axis=1), weights, preferred_element_type=F32)
    return out[:, :width] + out[:, width:]


def partner(me, step, tiles):
    if tiles & (tiles - 1):
        return lax.rem(me + tiles - step, tiles)
    other, bit = me, 1
    while bit < tiles:
        if step & bit:
            other = other + bit - 2 * bit * lax.rem(lax.div(me, bit), 2)
        bit *= 2
    return other


def batches_of(tiles):
    starts = [n for n in (0, 2) if n < tiles] + list(range(4, tiles, 4))
    return [range(a, b) for a, b in zip(starts, starts[1:] + [tiles])]


def weights_kernel(
    tiles, lags, slots, group, columns,
    pert_hbm, innov_hbm, rinv_hbm, tile_hbm, col_hbm, count_hbm, ens_hbm,
    turned, ens,
    move_sem,
    innov_ref, rinv_ref, tile_ref, col_ref, count_ref, load_sem,
    msg, snd, rcv, acc, to_left, to_right, from_left, from_right, mine, theirs,
    a2a_send, a2a_recv, halo_send, halo_recv, lag_send, lag_recv, product, edge, edge_rcv, edge_acc, edge_send, edge_recv, ready,
):
    members, own = pert_hbm.shape
    points = columns // SPACING
    half = points // 2
    radius = columns // 2
    pair = 2 * members
    sent = members + META // 2
    me = lax.axis_index("space")
    my_lag = lax.axis_index("lag")

    loads = [
        pltpu.make_async_copy(source, dest, load_sem.at[n])
        for n, (source, dest) in enumerate((
            (tile_hbm, tile_ref),
            (count_hbm, count_ref),
            (rinv_hbm, rinv_ref),
            (innov_hbm, innov_ref),
            (col_hbm, col_ref),
            (pert_hbm, msg.at[0:members]),
        ))
    ]
    for load in loads:
        load.start()
    barrier = pltpu.get_barrier_semaphore()
    batches = batches_of(tiles)
    blocks_of = BLOCKS if tiles % BLOCKS == 0 else 1
    wide = tiles // blocks_of
    mine_block, inner = lax.div(me, wide), lax.rem(me, wide)

    def rank_of(tile):
        block, place = lax.div(tile, wide), lax.rem(tile, wide)
        digits, bit = block, 1
        while bit < wide:
            digits = digits + lax.rem(lax.div(place, bit), 2)
            bit *= 2
        return digits * tiles + tile

    def before(a, b):
        return lax.div(b - a + span - 1, span)

    span = tiles * (tiles + blocks_of)
    my_rank = rank_of(me)
    ranks_of = [rank_of(jnp.int32(tile)) for tile in range(tiles)]
    earlier = sum(before(r, my_rank) for r in ranks_of)
    for peer in range(tiles - 1, -1, -1):
        @pl.when(my_rank < ranks_of[peer])
        def _(peer=peer):
            pl.semaphore_signal(barrier, inc=1, device_id={"space": peer})
    for step in range(1, lags):
        pl.semaphore_signal(barrier, inc=1, device_id={"lag": lax.rem(my_lag + step, lags)})

    for load in loads:
        load.wait()

    slot_id = lax.broadcasted_iota(jnp.int32, (1, own), 1)
    weight = jnp.where(slot_id < count_ref[0, 0], rinv_ref[...].astype(F32), 0.0)
    column = col_ref[...]
    col_hi = (column // BASE).astype(F32)
    col_lo = (column % BASE).astype(F32)
    row = lax.broadcasted_iota(jnp.int32, (META, own), 0)
    meta = jnp.where(row == 0, weight, 0.0)
    meta = jnp.where(row == 1, innov_ref[...].astype(F32), meta)
    meta = jnp.where(row == 2, col_hi, meta)
    meta = jnp.where(row == 3, col_lo, meta)
    msg[members:, :] = meta.astype(BF16)

    target = tile_ref[...]
    hits = jnp.where(target == lax.broadcasted_iota(jnp.int32, (tiles, own), 0), 1.0, 0.0)
    tri = jnp.where(
        lax.broadcasted_iota(jnp.int32, (LANES, LANES), 0)
        < lax.broadcasted_iota(jnp.int32, (LANES, LANES), 1),
        1.0, 0.0,
    ).astype(BF16)
    seen = jnp.zeros((tiles, 1), F32)
    ranks = []
    for b in range(own // LANES):
        block = hits[:, b * LANES : (b + 1) * LANES]
        ahead = jnp.dot(block.astype(BF16), tri, preferred_element_type=F32) + seen
        ranks.append(jnp.sum(ahead * block, axis=0, keepdims=True))
        seen = seen + jnp.sum(block, axis=1, keepdims=True)
    rank = jnp.concatenate(ranks, axis=1)
    place = lax.broadcasted_iota(jnp.int32, (slots, own), 0).astype(F32).astype(BF16)
    message = msg[...]

    def bucket(dest):
        wanted = jnp.where(target == dest, rank, -1.0).astype(BF16)
        chosen = jnp.where(place == wanted, jnp.ones((), BF16), jnp.zeros((), BF16))
        return lax.dot_general(message, chosen, NT, preferred_element_type=F32).astype(BF16)

    def a2a(peer):
        return pltpu.make_async_remote_copy(
            src_ref=snd.at[peer, 0:sent], dst_ref=rcv.at[step_of(peer), 0:sent],
            send_sem=a2a_send.at[0], recv_sem=a2a_recv.at[lax.div(step_of(peer), group)],
            device_id={"space": jnp.int32(peer)},
        )

    pl.semaphore_wait(barrier, earlier + lags - 1)
    my_batch = sum(lax.div(me + tiles - batch[0], tiles) for batch in batches[1:])
    for peer in range(tiles):
        @pl.when(ranks_of[peer] < my_rank)
        def _(peer=peer):
            pl.semaphore_signal(ready.at[my_batch], inc=1, device_id={"space": peer})

    def edge_copy(source):
        return pltpu.make_async_remote_copy(
            src_ref=edge.at[0:sent], dst_ref=edge_rcv.at[source, 0:sent],
            send_sem=edge_send.at[0], recv_sem=edge_recv.at[lax.div(source, group)],
            device_id={"space": 0 * me},
        )

    def step_of(peer):
        block, place = peer // wide, peer % wide
        if blocks_of == 4:
            across = lax.div(mine_block, 2) - block // 2
            beside = mine_block - block
            middle = lax.div(mine_block * (3 - mine_block), 2)
            turn = (1 - across * across) * beside * beside + across * across * (2 + middle)
        else:
            turn = lax.rem(mine_block + blocks_of - block, blocks_of)
        return turn * wide + partner(inner, place, wide)

    def send(peer):
        @pl.when(me != peer)
        def _():
            a2a(peer).start()

    for n, batch in enumerate(batches):
        for peer in batch:
            snd[peer] = bucket(peer)
        if n == 0:
            edge[...] = bucket(tiles - 1)
        later = sum(before(my_rank, ranks_of[peer]) for peer in batch)

        @pl.when(later > 0)
        def _(n=n, later=later):
            pl.semaphore_wait(ready.at[n], later)

        for peer in batch:
            send(peer)
        if n == 0:
            @pl.when(me > 0)
            def _():
                edge_copy(step_of(0)).start()
    for step in range(1, tiles):
        rcv[step, sent:] = jnp.zeros((members + META - sent, slots), BF16)

    ens_load = pltpu.make_async_copy(ens_hbm, ens, move_sem.at[0])
    ens_load.start()
    arrivals = list(range(tiles))

    def landed(place, sem, first):
        part = place.at[max(first, 1) : first + group, 0:sent]
        return pltpu.make_async_copy(part, part, sem.at[first // group])

    def partials(obs, ks, into, base, fresh):
        pert = obs[0:members].astype(F32)
        info = obs[members:].astype(F32)
        obs_weight = info[0:1]
        places = info[2:3] * BASE + info[3:4]
        for k in ks:
            center = float((k - half) * SPACING + SPACING // 2)
            taper = jnp.maximum(1.0 - jnp.abs(places - center) / radius, 0.0)
            rho = taper * taper * obs_weight
            scaled = (pert * rho).astype(BF16)
            part = lax.dot_general(obs, scaled, NT, preferred_element_type=F32)
            if fresh:
                into[k - base] = part
            else:
                into[k - base] += part

    for first in range(0, tiles, group):
        landed(rcv, a2a_recv, first).wait()
        obs = jnp.concatenate(
            [rcv[step] if step else snd[me] for step in arrivals[first : first + group]], axis=1
        )

        def moments(ks, obs=obs, first=first):
            partials(obs, ks, acc, 0, first == 0)

        @pl.when(me == 0)
        def _(first=first):
            landed(edge_rcv, edge_recv, first).wait()
            near = [
                edge_rcv[step] if step else edge[...] for step in arrivals[first : first + group]
            ]
            partials(
                jnp.concatenate(near, axis=1), range(points + half - 1, points + 2 * half),
                edge_acc, points + half - 1, first == 0,
            )

        if first + group < tiles:
            moments(range(points + 2 * half))

    lane = lax.broadcasted_iota(jnp.int32, (members, pair), 1)
    low = lane < members

    def joined(a, b, source=acc):
        return jnp.concatenate([source[a, 0:members], source[b, 0:members]], axis=1)

    def drives_of(a, b, source=acc):
        none = jnp.zeros((1, members), F32)
        return jnp.concatenate(
            [none if k is None else source[k, members + 1 : members + 2] for k in (a, b)], axis=1
        )

    left_copy = pltpu.make_async_remote_copy(
        src_ref=to_left, dst_ref=from_right, send_sem=halo_send.at[0], recv_sem=halo_recv.at[0],
        device_id={"space": lax.rem(me + tiles - 1, tiles)},
    )
    right_copy = pltpu.make_async_remote_copy(
        src_ref=to_right, dst_ref=from_left, send_sem=halo_send.at[1], recv_sem=halo_recv.at[1],
        device_id={"space": lax.rem(me + 1, tiles)},
    )

    fold = members // 2
    extra = members * (half // 4) + fold
    row = lax.broadcasted_iota(jnp.int32, (members, pair), 0)
    within = lax.rem(lane, members)

    def packed(single, ks, source=acc):
        first = [joined(ks[n], ks[n + 1], source) for n in range(0, half, 2)]
        ends = (None, single) if single < ks[0] else (single, None)
        vectors = [drives_of(ks[n], ks[n + 1], source) for n in range(0, half, 2)]
        vectors.append(drives_of(*ends, source))
        vectors += [
            jnp.sum(jnp.where(row == within, other, 0.0), axis=0, keepdims=True)
            for other in first[1::2]
        ]
        spare = -len(vectors) % 8
        if spare:
            vectors.append(jnp.zeros((spare, pair), F32))
        parts = [
            jnp.where(row <= within, first[n], first[n + 1]) for n in range(0, half // 2, 2)
        ]
        tail = jnp.concatenate(
            [source[single, 0:fold], source[single, fold:members]], axis=1
        )
        return jnp.concatenate([*parts, tail, *vectors], axis=0)

    def unpacked(ref):
        pairs = []
        for n in range(half // 4):
            part = ref[n * members : (n + 1) * members]
            flipped = jnp.concatenate([part[:, 0:members].T, part[:, members:].T], axis=1)
            pairs.append(jnp.where(row <= within, part, flipped))
            at = extra + half // 2 + 1 + n
            other = jnp.where(row == within, ref[at : at + 1], flipped)
            pairs.append(jnp.where(row > within, part, other))
        tail = ref[extra - fold : extra]
        corner = tail[:, 0:members].T[fold:]
        bottom = jnp.concatenate([corner, tail[:, members + fold :]], axis=1)
        single = jnp.concatenate([tail[:, 0:members], bottom], axis=0)
        return pairs, single, [ref[extra + n : extra + n + 1] for n in range(half // 2 + 1)]

    last = points + 2 * half - 1
    moments(range(half + 1))
    to_left[...] = packed(0, list(range(1, half + 1)))
    moments(range(last - half, last + 1))
    left_copy.start()
    to_right[...] = packed(last, list(range(last - half, last)))

    moments(range(half + 1, half + 3))

    @pl.when(me < tiles - 1)
    def _():
        right_copy.start()

    moments(range(half + 3, last - half))

    eye = jnp.where(
        lax.rem(lane, members) == lax.broadcasted_iota(jnp.int32, (members, pair), 0), 1.0, 0.0
    )
    mask_low = jnp.where(low, 1.0, 0.0).astype(BF16)
    mask_high = jnp.where(low, 0.0, 1.0).astype(BF16)

    def diagonal(x):
        return jnp.concatenate([x * mask_low, x * mask_high], axis=0)

    def blocks(x):
        hi, lo = halves(x)
        return stationary(diagonal(hi), diagonal(lo))


    count = (points + 2) // 2
    own_pairs = [joined(half - 1 + 2 * i, half + 2 * i) for i in range(count)]
    own_drives = [drives_of(half - 1 + 2 * i, half + 2 * i) for i in range(count)]
    left_copy.wait_recv()

    @pl.when(me > 0)
    def _():
        right_copy.wait_recv()

    @pl.when(me == 0)
    def _():
        from_left[...] = packed(half, list(range(half)), edge_acc)

    lefts, left_single, left_drives = unpacked(from_left)
    rights, right_single, right_drives = unpacked(from_right)

    grams = []
    for i in range(count):
        total = own_pairs[i] + (members - 1.0) * eye
        if i < half // 2:
            total = total + lefts[i]
        elif i == half // 2:
            total = total + jnp.concatenate([left_single, right_single], axis=1)
        else:
            total = total + rights[i - half // 2 - 1]
        grams.append(total)
    drives = [
        own_drives[i]
        + (left_drives[i] if i < half // 2 else 0.0)
        + (right_drives[i - half // 2 - 1] if i > half // 2 else 0.0)
        for i in range(count)
    ]
    drives[half // 2] += left_drives[half // 2] + right_drives[half // 2]

    states, scales = [], []
    row_low = lax.broadcasted_iota(jnp.int32, (1, pair), 1) < members
    for total in grams:
        squares = jnp.sum(total * total, axis=0, keepdims=True)
        sum_low = jnp.sum(jnp.where(row_low, squares, 0.0), axis=1, keepdims=True)
        sum_high = jnp.sum(jnp.where(row_low, 0.0, squares), axis=1, keepdims=True)
        scale = jnp.sqrt(jnp.where(row_low, sum_low, sum_high))
        scales.append(scale)
        states.append(total / scale)
    drives = [jnp.broadcast_to(drive, (THIN, pair)) for drive in drives]

    lowers = []
    for sweep in range(NS_ITERS):
        middles = [1.5 * eye - 0.5 * state for state in states]
        weights = [blocks(mid) for mid in middles]
        final = sweep == NS_ITERS - 1
        lefts = [
            ([] if final else [states[i]]) + ([lowers[i]] if sweep else []) + [drives[i]]
            for i in range(count)
        ]
        once = [times(jnp.concatenate(left, axis=0), w) for left, w in zip(lefts, weights)]
        lowers = [x[-THIN - members : -THIN] for x in once] if sweep else middles
        again = [
            x[-THIN:] if final else jnp.concatenate([x[0:members], x[-THIN:]], axis=0)
            for x in once
        ]
        twice = [times(left, w) for left, w in zip(again, weights)]
        states = [x[0:members] for x in twice]
        drives = [x[-THIN:] for x in twice]

    def centered(x):
        sum_low = jnp.sum(jnp.where(low[0:1], x, 0.0), axis=1, keepdims=True)
        sum_high = jnp.sum(jnp.where(low[0:1], 0.0, x), axis=1, keepdims=True)
        return x - jnp.where(low[0:1], sum_low, sum_high) / members

    results = []
    for i in range(count):
        root = lowers[i] / jnp.sqrt(scales[i])
        shift = drives[i][0:1] / scales[i]
        full = math.sqrt(members - 1.0) * root + shift
        results.append(centered(full) + 1.0 / members)
    for i in range(count):
        mine[i] = results[i]
        product[i] = results[i]

    def lag_copy(step):
        return pltpu.make_async_remote_copy(
            src_ref=mine, dst_ref=theirs.at[step - 1],
            send_sem=lag_send.at[step - 1], recv_sem=lag_recv.at[step - 1],
            device_id={"lag": lax.rem(my_lag + lags - step, lags)},
        )

    for step in range(1, lags):
        @pl.when(my_lag >= step)
        def _(step=step):
            lag_copy(step).start()
    for step in range(1, lags):
        @pl.when(my_lag + step < lags)
        def _(step=step):
            lag_copy(step).wait_recv()
            for i in range(count):
                product[i] = times(theirs[step - 1, i], blocks(product[i]))
    for i in range(count):
        both = product[i].astype(BF16)
        turned[i * pair : i * pair + members] = both[:, 0:members]
        turned[i * pair + members : (i + 1) * pair] = both[:, members:]
    ens_load.wait()

    gone = snd.at[1:tiles, 0:sent]
    pltpu.make_async_copy(gone, gone, a2a_send.at[0]).wait()
    left_copy.wait_send()

    @pl.when(me < tiles - 1)
    def _():
        right_copy.wait_send()

    @pl.when(me > 0)
    def _():
        edge_copy(step_of(0)).wait_send()

    for step in range(1, lags):
        @pl.when(my_lag >= step)
        def _(step=step):
            lag_copy(step).wait_send()


def apply_kernel(turned, ens, out_hbm, out, store_sem):
    members, columns = ens.shape
    points = columns // SPACING
    stores = []
    half_span = SPACING // 2
    for s in range(points + 1):
        start = max(s * SPACING - half_span, 0)
        stop = min(s * SPACING + half_span, columns)
        both = jnp.dot(
            turned[s * members : (s + 2) * members], ens[:, start:stop],
            preferred_element_type=F32,
        )
        along = lax.broadcasted_iota(jnp.int32, (1, stop - start), 1).astype(F32)
        second = (along + float(start - (s * SPACING - half_span))) / SPACING
        mixed = both[0:members] * (1.0 - second) + both[members:] * second
        out[:, start:stop] = mixed.astype(BF16)
        if s % 3 == 2:
            first = max((s - 2) * SPACING - half_span, 0)
            store = pltpu.make_async_copy(
                out.at[:, first:stop], out_hbm.at[:, first:stop], store_sem.at[s // 3]
            )
            store.start()
            stores.append(store)
    for store in stores:
        store.wait()


def per_device(ensemble, obs_pert, obs_innov, obs_rinv, obs_tile, obs_column, obs_count):
    members, columns = ensemble.shape[1:]
    own = obs_pert.shape[2]
    tiles, lags = lax.axis_size("space"), lax.axis_size("lag")
    slot_size = max(2, 2 * own // tiles)
    slots = -(-slot_size // LANES) * LANES
    group = 4
    points = columns // SPACING
    half = points // 2
    count = (points + 2) // 2
    pair = 2 * members
    rows = members + META
    vectors = half // 2 + 1 + half // 4
    side = (members * (half // 4) + members // 2 + -(-vectors // 8) * 8, pair)
    turned, held = pl.pallas_call(
        functools.partial(weights_kernel, tiles, lags, slots, group, columns),
        out_shape=(pltpu.VMEM((count * pair, members), BF16), pltpu.VMEM((members, columns), BF16)),
        in_specs=[pl.BlockSpec(memory_space=pltpu.HBM)] * 7,
        out_specs=[pl.BlockSpec(memory_space=pltpu.VMEM)] * 2,
        scratch_shapes=[
            pltpu.SemaphoreType.DMA((1,)),
            pltpu.VMEM((1, own), BF16),
            pltpu.VMEM((1, own), BF16),
            pltpu.VMEM((1, own), jnp.int32),
            pltpu.VMEM((1, own), jnp.int32),
            pltpu.SMEM((1, 1), jnp.int32),
            pltpu.SemaphoreType.DMA((6,)),
            pltpu.VMEM((rows, own), BF16),
            pltpu.VMEM((tiles, rows, slots), BF16),
            pltpu.VMEM((tiles, rows, slots), BF16),
            pltpu.VMEM((points + 2 * half, rows, members), F32),
            pltpu.VMEM(side, F32),
            pltpu.VMEM(side, F32),
            pltpu.VMEM(side, F32),
            pltpu.VMEM(side, F32),
            pltpu.VMEM((count, members, pair), F32),
            pltpu.VMEM((max(lags - 1, 1), count, members, pair), F32),
            pltpu.SemaphoreType.DMA((1,)),
            pltpu.SemaphoreType.DMA((-(-tiles // group),)),
            pltpu.SemaphoreType.DMA((2,)),
            pltpu.SemaphoreType.DMA((2,)),
            pltpu.SemaphoreType.DMA((max(lags - 1, 1),)),
            pltpu.SemaphoreType.DMA((max(lags - 1, 1),)),
            pltpu.VMEM((count, members, pair), F32),
            pltpu.VMEM((rows, slots), BF16),
            pltpu.VMEM((tiles, rows, slots), BF16),
            pltpu.VMEM((half + 1, rows, members), F32),
            pltpu.SemaphoreType.DMA((1,)),
            pltpu.SemaphoreType.DMA((-(-tiles // group),)),
            pltpu.SemaphoreType.REGULAR((len(batches_of(tiles)),)),
        ],
        compiler_params=pltpu.CompilerParams(
            collective_id=0, has_side_effects=True, vmem_limit_bytes=LIMIT
        ),
        name="ensemble_weights",
    )(*(
        x if x.size == 1 else pltpu.with_memory_space_constraint(x, pltpu.HBM)
        for x in (
            obs_pert[0], obs_innov, obs_rinv, obs_tile[:, :, 0], obs_column, obs_count, ensemble[0]
        )
    ))
    analysis = pl.pallas_call(
        apply_kernel,
        out_shape=jax.ShapeDtypeStruct((members, columns), BF16),
        in_specs=[pl.BlockSpec(memory_space=pltpu.VMEM)] * 2,
        out_specs=pl.BlockSpec(memory_space=pltpu.HBM),
        scratch_shapes=[
            pltpu.VMEM((members, columns), BF16),
            pltpu.SemaphoreType.DMA(((points + 1) // 3,)),
        ],
        compiler_params=pltpu.CompilerParams(vmem_limit_bytes=LIMIT),
        name="apply_weights",
    )(turned, held)
    return analysis[None]


def solution(mesh):
    return jax.shard_map(
        per_device,
        mesh=mesh,
        in_specs=(
            P("lag", None, "space"),
            P("lag", None, "space"),
            P("lag", "space"),
            P("lag", "space"),
            P("lag", "space", None),
            P("lag", "space"),
            P("lag", "space"),
        ),
        out_specs=P("lag", None, "space"),
        check_vma=False,
    )
```

```python
import functools
import math

import jax
import jax.numpy as jnp
from jax import lax
from jax.experimental import pallas as pl
from jax.experimental.pallas import tpu as pltpu
from jax.sharding import PartitionSpec as P

SPACING = 512
NS_ITERS = 6
THIN = 16
BLOCKS = 4
LIMIT = 24 * 1024 * 1024
LANES = 128
META = 16
BASE = 64
F32 = jnp.float32
BF16 = jnp.bfloat16
NT = (((1,), (1,)), ((), ()))


def halves(x):
    hi = x.astype(BF16)
    return hi, (x - hi.astype(F32)).astype(BF16)


def stationary(hi, lo):
    row = jnp.concatenate([hi, lo], axis=1)
    return jnp.concatenate([row, row], axis=0)


def times(left, weights):
    width = weights.shape[1] // 2
    hi, lo = halves(left)
    out = jnp.dot(jnp.concatenate([hi, lo], axis=1), weights, preferred_element_type=F32)
    return out[:, :width] + out[:, width:]


def mixed(a, b, width):
    if width & (width - 1):
        return lax.rem(a + width - b, width)
    out, bit = 0, 1
    while bit < width:
        one, two = lax.rem(lax.div(a, bit), 2), lax.rem(lax.div(b, bit), 2)
        out = out + bit * (one + two - 2 * one * two)
        bit *= 2
    return out


def batches_of(tiles):
    starts = [n for n in (0, 2) if n < tiles] + list(range(4, tiles, 4))
    return [range(a, b) for a, b in zip(starts, starts[1:] + [tiles])]


def weights_kernel(
    tiles, lags, slots, group, columns,
    pert_hbm, innov_hbm, rinv_hbm, tile_hbm, col_hbm, count_hbm, ens_hbm,
    turned, ens,
    move_sem,
    innov_ref, rinv_ref, tile_ref, col_ref, count_ref, load_sem,
    msg, snd, rcv, snd_meta, rcv_meta, acc, to_left, to_right, from_left, from_right, mine, theirs,
    a2a_send, a2a_recv, halo_send, halo_recv, lag_send, lag_recv, product, edge, edge_rcv, edge_acc, edge_send, edge_recv, ready,
):
    members, own = pert_hbm.shape
    points = columns // SPACING
    half = points // 2
    radius = columns // 2
    pair = 2 * members
    sent = members + META // 2
    me = lax.axis_index("space")
    my_lag = lax.axis_index("lag")

    loads = [
        pltpu.make_async_copy(source, dest, load_sem.at[n])
        for n, (source, dest) in enumerate((
            (tile_hbm, tile_ref),
            (count_hbm, count_ref),
            (rinv_hbm, rinv_ref),
            (innov_hbm, innov_ref),
            (col_hbm, col_ref),
            (pert_hbm, msg.at[0:members]),
        ))
    ]
    for load in loads:
        load.start()
    barrier = pltpu.get_barrier_semaphore()
    batches = batches_of(tiles)
    blocks_of = BLOCKS
    wide = tiles // blocks_of
    mine_block, inner = lax.div(me, wide), lax.rem(me, wide)

    def rank_of(tile):
        block, place = lax.div(tile, wide), lax.rem(tile, wide)
        digits, bit = block, 1
        while bit < wide:
            digits = digits + lax.rem(lax.div(place, bit), 2)
            bit *= 2
        return digits * tiles + tile

    def before(a, b):
        return lax.div(b - a + span - 1, span)

    span = tiles * (tiles + blocks_of)
    my_rank = rank_of(me)
    ranks_of = [rank_of(jnp.int32(tile)) for tile in range(tiles)]
    earlier = sum(before(r, my_rank) for r in ranks_of)
    for peer in range(tiles - 1, -1, -1):
        @pl.when(my_rank < ranks_of[peer])
        def _(peer=peer):
            pl.semaphore_signal(barrier, inc=1, device_id={"space": peer})
    for step in range(1, lags):
        pl.semaphore_signal(barrier, inc=1, device_id={"lag": lax.rem(my_lag + step, lags)})

    for load in loads:
        load.wait()

    slot_id = lax.broadcasted_iota(jnp.int32, (1, own), 1)
    weight = jnp.where(slot_id < count_ref[0, 0], rinv_ref[...].astype(F32), 0.0)
    column = col_ref[...]
    col_hi = (column // BASE).astype(F32)
    col_lo = (column % BASE).astype(F32)
    row = lax.broadcasted_iota(jnp.int32, (META, own), 0)
    meta = jnp.where(row == 0, weight, 0.0)
    meta = jnp.where(row == 1, innov_ref[...].astype(F32), meta)
    meta = jnp.where(row == 2, col_hi, meta)
    meta = jnp.where(row == 3, col_lo, meta)
    msg[members:, :] = meta.astype(BF16)

    target = tile_ref[...]
    hits = jnp.where(target == lax.broadcasted_iota(jnp.int32, (tiles, own), 0), 1.0, 0.0)
    tri = jnp.where(
        lax.broadcasted_iota(jnp.int32, (LANES, LANES), 0)
        < lax.broadcasted_iota(jnp.int32, (LANES, LANES), 1),
        1.0, 0.0,
    ).astype(BF16)
    seen = jnp.zeros((tiles, 1), F32)
    ranks = []
    for b in range(own // LANES):
        block = hits[:, b * LANES : (b + 1) * LANES]
        ahead = jnp.dot(block.astype(BF16), tri, preferred_element_type=F32) + seen
        ranks.append(jnp.sum(ahead * block, axis=0, keepdims=True))
        seen = seen + jnp.sum(block, axis=1, keepdims=True)
    rank = jnp.concatenate(ranks, axis=1)
    place = lax.broadcasted_iota(jnp.int32, (slots, own), 0).astype(F32).astype(BF16)
    message = msg[...]

    def bucket(dest):
        wanted = jnp.where(target == dest, rank, -1.0).astype(BF16)
        chosen = jnp.where(place == wanted, jnp.ones((), BF16), jnp.zeros((), BF16))
        return lax.dot_general(message, chosen, NT, preferred_element_type=F32).astype(BF16)

    def a2a(peer):
        step = step_of(peer)
        return [
            pltpu.make_async_remote_copy(
                src_ref=source.at[peer], dst_ref=dest.at[step],
                send_sem=a2a_send.at[n], recv_sem=a2a_recv.at[n, lax.div(step, group)],
                device_id={"space": peer},
            )
            for n, (source, dest) in enumerate(((snd, rcv), (snd_meta, rcv_meta)))
        ]

    pl.semaphore_wait(barrier, earlier + lags - 1)
    my_batch = sum(lax.div(me + tiles - batch[0], tiles) for batch in batches[1:])
    for peer in range(tiles):
        @pl.when(ranks_of[peer] < my_rank)
        def _(peer=peer):
            pl.semaphore_signal(ready.at[my_batch], inc=1, device_id={"space": peer})

    def edge_copy(source):
        return pltpu.make_async_remote_copy(
            src_ref=edge.at[0:sent], dst_ref=edge_rcv.at[source, 0:sent],
            send_sem=edge_send.at[0], recv_sem=edge_recv.at[lax.div(source, group)],
            device_id={"space": 0 * me},
        )

    def step_of(peer):
        block, place = lax.div(peer, wide), lax.rem(peer, wide)
        across = lax.div(mine_block, 2) - lax.div(block, 2)
        beside = mine_block - block
        middle = lax.div(mine_block * (3 - mine_block), 2)
        turn = (1 - across * across) * beside * beside + across * across * (2 + middle)
        return turn * wide + mixed(inner, place, wide)

    def send(peer):
        @pl.when(me != peer)
        def _():
            for copy in a2a(peer):
                copy.start()

    lower = 1 - lax.div(mine_block, 2)
    fills, plans = [], []
    for n, batch in enumerate(batches):
        block = batch[0] // wide
        shift = (1 - lower) * (4 - 2 * block) * wide if block % 2 else jnp.int32(0)
        peers = [jnp.int32(tile) + shift for tile in batch]
        def fill(n=n, peers=peers):
            for peer in peers:
                filled = bucket(peer)
                snd[peer] = filled[0:members]
                snd_meta[peer] = filled[members : members + META // 4]
            if n == len(batches) - 1:
                edge[...] = bucket(tiles - 1)

        fills.append(fill)
        plans.append((peers, shift))
    fills[0]()
    pl.when(mine_block == 0)(lambda: [fill() for fill in fills[1:]] and None)
    for n, (peers, shift) in enumerate(plans):
        if n:
            pl.when(mine_block > 0)(fills[n])
        later = sum(before(my_rank, rank_of(peer)) for peer in peers)

        @pl.when(later > 0)
        def _(n=n, later=later, shift=shift):
            pl.semaphore_wait(ready.at[n + lax.div(shift, 4)], later)

        for peer in peers:
            send(peer)
        if n == len(batches) - 1:
            @pl.when(me > 0)
            def _():
                edge_copy(step_of(me * 0)).start()
    ens_load = pltpu.make_async_copy(ens_hbm, ens, move_sem.at[0])
    ens_load.start()
    arrivals = list(range(tiles))

    def landed(place, sem, first):
        part = place.at[max(first, 1) : first + group]
        return pltpu.make_async_copy(part, part, sem)

    def partials(obs, ks, into, base, fresh):
        pert = obs[0:members].astype(F32)
        info = obs[members:].astype(F32)
        obs_weight = info[0:1]
        places = info[2:3] * BASE + info[3:4]
        for k in ks:
            center = float((k - half) * SPACING + SPACING // 2)
            taper = jnp.maximum(1.0 - jnp.abs(places - center) / radius, 0.0)
            rho = taper * taper * obs_weight
            scaled = (pert * rho).astype(BF16)
            part = lax.dot_general(obs, scaled, NT, preferred_element_type=F32)
            if fresh:
                into[k - base] = part
            else:
                into[k - base] += part

    for first in range(0, tiles, group):
        landed(rcv, a2a_recv.at[0, first // group], first).wait()
        landed(rcv_meta, a2a_recv.at[1, first // group], first).wait()
        steps = arrivals[first : first + group]
        obs = jnp.concatenate(
            [
                jnp.concatenate([rcv[step] if step else snd[me] for step in steps], axis=1),
                jnp.concatenate(
                    [rcv_meta[step] if step else snd_meta[me] for step in steps], axis=1
                ),
                jnp.zeros((META - META // 4, group * slots), BF16),
            ],
            axis=0,
        )

        def moments(ks, obs=obs, first=first):
            partials(obs, ks, acc, 0, first == 0)

        if first + group < tiles:
            moments(range(points + 2 * half))

    lane = lax.broadcasted_iota(jnp.int32, (members, pair), 1)
    low = lane < members

    def joined(a, b, source=acc):
        return jnp.concatenate([source[a, 0:members], source[b, 0:members]], axis=1)

    def drives_of(a, b, source=acc):
        none = jnp.zeros((1, members), F32)
        return jnp.concatenate(
            [none if k is None else source[k, members + 1 : members + 2] for k in (a, b)], axis=1
        )

    left_copy = pltpu.make_async_remote_copy(
        src_ref=to_left, dst_ref=from_right, send_sem=halo_send.at[0], recv_sem=halo_recv.at[0],
        device_id={"space": lax.rem(me + tiles - 1, tiles)},
    )
    right_copy = pltpu.make_async_remote_copy(
        src_ref=to_right, dst_ref=from_left, send_sem=halo_send.at[1], recv_sem=halo_recv.at[1],
        device_id={"space": lax.rem(me + 1, tiles)},
    )

    fold = members // 2
    extra = members * (half // 4) + fold
    row = lax.broadcasted_iota(jnp.int32, (members, pair), 0)
    within = lax.rem(lane, members)

    def packed(single, ks, source=acc):
        first = [joined(ks[n], ks[n + 1], source) for n in range(0, half, 2)]
        ends = (None, single) if single < ks[0] else (single, None)
        vectors = [drives_of(ks[n], ks[n + 1], source) for n in range(0, half, 2)]
        vectors.append(drives_of(*ends, source))
        vectors += [
            jnp.sum(jnp.where(row == within, other, 0.0), axis=0, keepdims=True)
            for other in first[1::2]
        ]
        spare = -len(vectors) % 8
        if spare:
            vectors.append(jnp.zeros((spare, pair), F32))
        parts = [
            jnp.where(row <= within, first[n], first[n + 1]) for n in range(0, half // 2, 2)
        ]
        tail = jnp.concatenate(
            [source[single, 0:fold], source[single, fold:members]], axis=1
        )
        return jnp.concatenate([*parts, tail, *vectors], axis=0)

    def unpacked(ref):
        pairs = []
        for n in range(half // 4):
            part = ref[n * members : (n + 1) * members]
            flipped = jnp.concatenate([part[:, 0:members].T, part[:, members:].T], axis=1)
            pairs.append(jnp.where(row <= within, part, flipped))
            at = extra + half // 2 + 1 + n
            other = jnp.where(row == within, ref[at : at + 1], flipped)
            pairs.append(jnp.where(row > within, part, other))
        tail = ref[extra - fold : extra]
        corner = tail[:, 0:members].T[fold:]
        bottom = jnp.concatenate([corner, tail[:, members + fold :]], axis=1)
        single = jnp.concatenate([tail[:, 0:members], bottom], axis=0)
        return pairs, single, [ref[extra + n : extra + n + 1] for n in range(half // 2 + 1)]

    last = points + 2 * half - 1
    moments(range(half + 1))
    to_left[...] = packed(0, list(range(1, half + 1)))
    moments(range(last - half, last + 1))
    left_copy.start()
    to_right[...] = packed(last, list(range(last - half, last)))

    moments(range(half + 1, half + 3))

    @pl.when(me < tiles - 1)
    def _():
        right_copy.start()

    moments(range(half + 3, last - half))

    eye = jnp.where(
        lax.rem(lane, members) == lax.broadcasted_iota(jnp.int32, (members, pair), 0), 1.0, 0.0
    )
    mask_low = jnp.where(low, 1.0, 0.0).astype(BF16)
    mask_high = jnp.where(low, 0.0, 1.0).astype(BF16)

    def diagonal(x):
        return jnp.concatenate([x * mask_low, x * mask_high], axis=0)

    def blocks(x):
        hi, lo = halves(x)
        return stationary(diagonal(hi), diagonal(lo))


    count = (points + 2) // 2
    own_pairs = [joined(half - 1 + 2 * i, half + 2 * i) for i in range(count)]
    own_drives = [drives_of(half - 1 + 2 * i, half + 2 * i) for i in range(count)]
    @pl.when(me == 0)
    def _():
        for first in range(0, tiles, group):
            landed(edge_rcv.at[:, 0:sent], edge_recv.at[first // group], first).wait()
            near = [
                edge_rcv[step] if step else edge[...] for step in arrivals[first : first + group]
            ]
            partials(
                jnp.concatenate(near, axis=1), range(points + half - 1, points + 2 * half),
                edge_acc, points + half - 1, first == 0,
            )
        from_left[...] = packed(half, list(range(half)), edge_acc)

    left_copy.wait_recv()

    @pl.when(me > 0)
    def _():
        right_copy.wait_recv()

    lefts, left_single, left_drives = unpacked(from_left)
    rights, right_single, right_drives = unpacked(from_right)

    grams = []
    for i in range(count):
        total = own_pairs[i] + (members - 1.0) * eye
        if i < half // 2:
            total = total + lefts[i]
        elif i == half // 2:
            total = total + jnp.concatenate([left_single, right_single], axis=1)
        else:
            total = total + rights[i - half // 2 - 1]
        grams.append(total)
    drives = [
        own_drives[i]
        + (left_drives[i] if i < half // 2 else 0.0)
        + (right_drives[i - half // 2 - 1] if i > half // 2 else 0.0)
        for i in range(count)
    ]
    drives[half // 2] += left_drives[half // 2] + right_drives[half // 2]

    states, scales = [], []
    row_low = lax.broadcasted_iota(jnp.int32, (1, pair), 1) < members
    for total in grams:
        squares = jnp.sum(total * total, axis=0, keepdims=True)
        sum_low = jnp.sum(jnp.where(row_low, squares, 0.0), axis=1, keepdims=True)
        sum_high = jnp.sum(jnp.where(row_low, 0.0, squares), axis=1, keepdims=True)
        scale = jnp.sqrt(jnp.where(row_low, sum_low, sum_high))
        scales.append(scale)
        states.append(total / scale)
    drives = [jnp.broadcast_to(drive, (THIN, pair)) for drive in drives]

    lowers = []
    for sweep in range(NS_ITERS):
        middles = [1.5 * eye - 0.5 * state for state in states]
        weights = [blocks(mid) for mid in middles]
        final = sweep == NS_ITERS - 1
        lefts = [
            ([] if final else [states[i]]) + ([lowers[i]] if sweep else []) + [drives[i]]
            for i in range(count)
        ]
        once = [times(jnp.concatenate(left, axis=0), w) for left, w in zip(lefts, weights)]
        lowers = [x[-THIN - members : -THIN] for x in once] if sweep else middles
        again = [
            x[-THIN:] if final else jnp.concatenate([x[0:members], x[-THIN:]], axis=0)
            for x in once
        ]
        twice = [times(left, w) for left, w in zip(again, weights)]
        states = [x[0:members] for x in twice]
        drives = [x[-THIN:] for x in twice]

    def centered(x):
        sum_low = jnp.sum(jnp.where(low[0:1], x, 0.0), axis=1, keepdims=True)
        sum_high = jnp.sum(jnp.where(low[0:1], 0.0, x), axis=1, keepdims=True)
        return x - jnp.where(low[0:1], sum_low, sum_high) / members

    results = []
    for i in range(count):
        root = lowers[i] / jnp.sqrt(scales[i])
        shift = drives[i][0:1] / scales[i]
        full = math.sqrt(members - 1.0) * root + shift
        results.append(centered(full) + 1.0 / members)
    for i in range(count):
        mine[i] = results[i]
        product[i] = results[i]

    def lag_copy(step):
        return pltpu.make_async_remote_copy(
            src_ref=mine, dst_ref=theirs.at[step - 1],
            send_sem=lag_send.at[step - 1], recv_sem=lag_recv.at[step - 1],
            device_id={"lag": lax.rem(my_lag + lags - step, lags)},
        )

    for step in range(1, lags):
        @pl.when(my_lag >= step)
        def _(step=step):
            lag_copy(step).start()
    for step in range(1, lags):
        @pl.when(my_lag + step < lags)
        def _(step=step):
            lag_copy(step).wait_recv()
            for i in range(count):
                product[i] = times(theirs[step - 1, i], blocks(product[i]))
    for i in range(count):
        both = product[i].astype(BF16)
        turned[i * pair : i * pair + members] = both[:, 0:members]
        turned[i * pair + members : (i + 1) * pair] = both[:, members:]
    ens_load.wait()

    for n, source in enumerate((snd, snd_meta)):
        gone = source.at[1:tiles]
        pltpu.make_async_copy(gone, gone, a2a_send.at[n]).wait()
    left_copy.wait_send()

    @pl.when(me < tiles - 1)
    def _():
        right_copy.wait_send()

    @pl.when(me > 0)
    def _():
        edge_copy(step_of(me * 0)).wait_send()

    for step in range(1, lags):
        @pl.when(my_lag >= step)
        def _(step=step):
            lag_copy(step).wait_send()


def apply_kernel(turned, ens, out_hbm, out, store_sem):
    members, columns = ens.shape
    points = columns // SPACING
    stores = []
    half_span = SPACING // 2
    for s in range(points + 1):
        start = max(s * SPACING - half_span, 0)
        stop = min(s * SPACING + half_span, columns)
        both = jnp.dot(
            turned[s * members : (s + 2) * members], ens[:, start:stop],
            preferred_element_type=F32,
        )
        along = lax.broadcasted_iota(jnp.int32, (1, stop - start), 1).astype(F32)
        second = (along + float(start - (s * SPACING - half_span))) / SPACING
        mixed = both[0:members] * (1.0 - second) + both[members:] * second
        out[:, start:stop] = mixed.astype(BF16)
        if s % 3 == 2:
            first = max((s - 2) * SPACING - half_span, 0)
            store = pltpu.make_async_copy(
                out.at[:, first:stop], out_hbm.at[:, first:stop], store_sem.at[s // 3]
            )
            store.start()
            stores.append(store)
    for store in stores:
        store.wait()


def per_device(ensemble, obs_pert, obs_innov, obs_rinv, obs_tile, obs_column, obs_count):
    members, columns = ensemble.shape[1:]
    own = obs_pert.shape[2]
    tiles, lags = lax.axis_size("space"), lax.axis_size("lag")
    slot_size = max(2, 2 * own // tiles)
    slots = -(-slot_size // LANES) * LANES
    group = 4
    points = columns // SPACING
    half = points // 2
    count = (points + 2) // 2
    pair = 2 * members
    rows = members + META
    vectors = half // 2 + 1 + half // 4
    side = (members * (half // 4) + members // 2 + -(-vectors // 8) * 8, pair)
    turned, held = pl.pallas_call(
        functools.partial(weights_kernel, tiles, lags, slots, group, columns),
        out_shape=(pltpu.VMEM((count * pair, members), BF16), pltpu.VMEM((members, columns), BF16)),
        in_specs=[pl.BlockSpec(memory_space=pltpu.HBM)] * 7,
        out_specs=[pl.BlockSpec(memory_space=pltpu.VMEM)] * 2,
        scratch_shapes=[
            pltpu.SemaphoreType.DMA((1,)),
            pltpu.VMEM((1, own), BF16),
            pltpu.VMEM((1, own), BF16),
            pltpu.VMEM((1, own), jnp.int32),
            pltpu.VMEM((1, own), jnp.int32),
            pltpu.SMEM((1, 1), jnp.int32),
            pltpu.SemaphoreType.DMA((6,)),
            pltpu.VMEM((rows, own), BF16),
            pltpu.VMEM((tiles, members, slots), BF16),
            pltpu.VMEM((tiles, members, slots), BF16),
            pltpu.VMEM((tiles, META // 4, slots), BF16),
            pltpu.VMEM((tiles, META // 4, slots), BF16),
            pltpu.VMEM((points + 2 * half, rows, members), F32),
            pltpu.VMEM(side, F32),
            pltpu.VMEM(side, F32),
            pltpu.VMEM(side, F32),
            pltpu.VMEM(side, F32),
            pltpu.VMEM((count, members, pair), F32),
            pltpu.VMEM((max(lags - 1, 1), count, members, pair), F32),
            pltpu.SemaphoreType.DMA((2,)),
            pltpu.SemaphoreType.DMA((2, -(-tiles // group))),
            pltpu.SemaphoreType.DMA((2,)),
            pltpu.SemaphoreType.DMA((2,)),
            pltpu.SemaphoreType.DMA((max(lags - 1, 1),)),
            pltpu.SemaphoreType.DMA((max(lags - 1, 1),)),
            pltpu.VMEM((count, members, pair), F32),
            pltpu.VMEM((rows, slots), BF16),
            pltpu.VMEM((tiles, rows, slots), BF16),
            pltpu.VMEM((half + 1, rows, members), F32),
            pltpu.SemaphoreType.DMA((1,)),
            pltpu.SemaphoreType.DMA((-(-tiles // group),)),
            pltpu.SemaphoreType.REGULAR((len(batches_of(tiles)),)),
        ],
        compiler_params=pltpu.CompilerParams(
            collective_id=0, has_side_effects=True, vmem_limit_bytes=LIMIT
        ),
        name="ensemble_weights",
    )(*(
        x if x.size == 1 else pltpu.with_memory_space_constraint(x, pltpu.HBM)
        for x in (
            obs_pert[0], obs_innov, obs_rinv, obs_tile[:, :, 0], obs_column, obs_count, ensemble[0]
        )
    ))
    analysis = pl.pallas_call(
        apply_kernel,
        out_shape=jax.ShapeDtypeStruct((members, columns), BF16),
        in_specs=[pl.BlockSpec(memory_space=pltpu.VMEM)] * 2,
        out_specs=pl.BlockSpec(memory_space=pltpu.HBM),
        scratch_shapes=[
            pltpu.VMEM((members, columns), BF16),
            pltpu.SemaphoreType.DMA(((points + 1) // 3,)),
        ],
        compiler_params=pltpu.CompilerParams(vmem_limit_bytes=LIMIT),
        name="apply_weights",
    )(turned, held)
    return analysis[None]


def solution(mesh):
    return jax.shard_map(
        per_device,
        mesh=mesh,
        in_specs=(
            P("lag", None, "space"),
            P("lag", None, "space"),
            P("lag", "space"),
            P("lag", "space"),
            P("lag", "space", None),
            P("lag", "space"),
            P("lag", "space"),
        ),
        out_specs=P("lag", None, "space"),
        check_vma=False,
    )
```

```python
import functools
import math

import jax
import jax.numpy as jnp
from jax import lax
from jax.experimental import pallas as pl
from jax.experimental.pallas import tpu as pltpu
from jax.sharding import PartitionSpec as P

SPACING = 512
NS_ITERS = 6
TAIL = 2
THIN = 16
BLOCKS = 4
LIMIT = 24 * 1024 * 1024
LANES = 128
META = 16
BASE = 64
F32 = jnp.float32
BF16 = jnp.bfloat16
NT = (((1,), (1,)), ((), ()))


def halves(x):
    hi = x.astype(BF16)
    return hi, (x - hi.astype(F32)).astype(BF16)


def stationary(hi, lo):
    row = jnp.concatenate([hi, lo], axis=1)
    return jnp.concatenate([row, row], axis=0)


def times(left, weights):
    width = weights.shape[1] // 2
    hi, lo = halves(left)
    out = jnp.dot(jnp.concatenate([hi, lo], axis=1), weights, preferred_element_type=F32)
    return out[:, :width] + out[:, width:]


def mixed(a, b, width):
    if width & (width - 1):
        return lax.rem(a + width - b, width)
    out, bit = 0, 1
    while bit < width:
        one, two = lax.rem(lax.div(a, bit), 2), lax.rem(lax.div(b, bit), 2)
        out = out + bit * (one + two - 2 * one * two)
        bit *= 2
    return out


def batches_of(tiles):
    starts = [n for n in (0, 2) if n < tiles] + list(range(4, tiles, 4))
    return [range(a, b) for a, b in zip(starts, starts[1:] + [tiles])]


def weights_kernel(
    tiles, lags, slots, group, columns,
    pert_hbm, innov_hbm, rinv_hbm, tile_hbm, col_hbm, count_hbm, ens_hbm,
    turned, ens,
    move_sem,
    innov_ref, rinv_ref, tile_ref, col_ref, count_ref, load_sem,
    msg, snd, rcv, snd_meta, rcv_meta, acc, to_left, to_right, from_left, from_right, mine, theirs,
    a2a_send, a2a_recv, halo_send, halo_recv, lag_send, lag_recv, product, edge, edge_rcv, edge_acc, edge_send, edge_recv, ready,
):
    members, own = pert_hbm.shape
    points = columns // SPACING
    half = points // 2
    radius = columns // 2
    pair = 2 * members
    sent = members + META // 2
    me = lax.axis_index("space")
    my_lag = lax.axis_index("lag")

    loads = [
        pltpu.make_async_copy(source, dest, load_sem.at[n])
        for n, (source, dest) in enumerate((
            (tile_hbm, tile_ref),
            (count_hbm, count_ref),
            (rinv_hbm, rinv_ref),
            (innov_hbm, innov_ref),
            (col_hbm, col_ref),
            (pert_hbm, msg.at[0:members]),
        ))
    ]
    for load in loads:
        load.start()
    barrier = pltpu.get_barrier_semaphore()
    batches = batches_of(tiles)
    blocks_of = BLOCKS
    wide = tiles // blocks_of
    mine_block, inner = lax.div(me, wide), lax.rem(me, wide)

    def rank_of(tile):
        block, place = lax.div(tile, wide), lax.rem(tile, wide)
        digits, bit = block, 1
        while bit < wide:
            digits = digits + lax.rem(lax.div(place, bit), 2)
            bit *= 2
        return digits * tiles + tile

    def before(a, b):
        return lax.div(b - a + span - 1, span)

    span = tiles * (tiles + blocks_of)
    my_rank = rank_of(me)
    ranks_of = [rank_of(jnp.int32(tile)) for tile in range(tiles)]
    earlier = sum(before(r, my_rank) for r in ranks_of)
    for peer in range(tiles - 1, -1, -1):
        @pl.when(my_rank < ranks_of[peer])
        def _(peer=peer):
            pl.semaphore_signal(barrier, inc=1, device_id={"space": peer})
    for step in range(1, lags):
        pl.semaphore_signal(barrier, inc=1, device_id={"lag": lax.rem(my_lag + step, lags)})

    loads[0].wait()

    target = tile_ref[...]
    hits = jnp.where(target == lax.broadcasted_iota(jnp.int32, (tiles, own), 0), 1.0, 0.0)
    tri = jnp.where(
        lax.broadcasted_iota(jnp.int32, (LANES, LANES), 0)
        < lax.broadcasted_iota(jnp.int32, (LANES, LANES), 1),
        1.0, 0.0,
    ).astype(BF16)
    seen = jnp.zeros((tiles, 1), F32)
    ranks = []
    for b in range(own // LANES):
        block = hits[:, b * LANES : (b + 1) * LANES]
        ahead = jnp.dot(block.astype(BF16), tri, preferred_element_type=F32) + seen
        ranks.append(jnp.sum(ahead * block, axis=0, keepdims=True))
        seen = seen + jnp.sum(block, axis=1, keepdims=True)
    rank = jnp.concatenate(ranks, axis=1)
    place = lax.broadcasted_iota(jnp.int32, (slots, own), 0).astype(F32).astype(BF16)

    def bucket(dest):
        wanted = jnp.where(target == dest, rank, -1.0).astype(BF16)
        chosen = jnp.where(place == wanted, jnp.ones((), BF16), jnp.zeros((), BF16))
        return lax.dot_general(message, chosen, NT, preferred_element_type=F32).astype(BF16)

    def a2a(peer):
        step = step_of(peer)
        return [
            pltpu.make_async_remote_copy(
                src_ref=source.at[peer], dst_ref=dest.at[step],
                send_sem=a2a_send.at[n], recv_sem=a2a_recv.at[n, lax.div(step, group) + lax.div(step, tiles - TAIL)],
                device_id={"space": peer},
            )
            for n, (source, dest) in enumerate(((snd, rcv), (snd_meta, rcv_meta)))
        ]

    pl.semaphore_wait(barrier, earlier + lags - 1)
    my_batch = sum(lax.div(me + tiles - batch[0], tiles) for batch in batches[1:])
    for peer in range(tiles):
        @pl.when(ranks_of[peer] < my_rank)
        def _(peer=peer):
            pl.semaphore_signal(ready.at[my_batch], inc=1, device_id={"space": peer})

    def edge_copy(source):
        return pltpu.make_async_remote_copy(
            src_ref=edge.at[0:sent], dst_ref=edge_rcv.at[source, 0:sent],
            send_sem=edge_send.at[0], recv_sem=edge_recv.at[lax.div(source, group)],
            device_id={"space": 0 * me},
        )

    def step_of(peer):
        block, place = lax.div(peer, wide), lax.rem(peer, wide)
        across = lax.div(mine_block, 2) - lax.div(block, 2)
        beside = mine_block - block
        middle = lax.div(mine_block * (3 - mine_block), 2)
        turn = (1 - across * across) * beside * beside + across * across * (2 + middle)
        return turn * wide + mixed(inner, place, wide)

    def send(peer):
        @pl.when(me != peer)
        def _():
            for copy in a2a(peer):
                copy.start()

    for load in loads[1:]:
        load.wait()
    slot_id = lax.broadcasted_iota(jnp.int32, (1, own), 1)
    weight = jnp.where(slot_id < count_ref[0, 0], rinv_ref[...].astype(F32), 0.0)
    column = col_ref[...]
    col_hi = (column // BASE).astype(F32)
    col_lo = (column % BASE).astype(F32)
    row = lax.broadcasted_iota(jnp.int32, (META, own), 0)
    meta = jnp.where(row == 0, weight, 0.0)
    meta = jnp.where(row == 1, innov_ref[...].astype(F32), meta)
    meta = jnp.where(row == 2, col_hi, meta)
    meta = jnp.where(row == 3, col_lo, meta)
    msg[members:, :] = meta.astype(BF16)

    message = msg[...]
    lower = 1 - lax.div(mine_block, 2)
    fills, plans = [], []
    for n, batch in enumerate(batches):
        block = batch[0] // wide
        shift = (1 - lower) * (4 - 2 * block) * wide if block % 2 else jnp.int32(0)
        peers = [jnp.int32(tile) + shift for tile in batch]
        def fill(n=n, peers=peers):
            for peer in peers:
                filled = bucket(peer)
                snd[peer] = filled[0:members]
                snd_meta[peer] = filled[members : members + META // 4]
            if n == len(batches) - 1:
                edge[...] = bucket(tiles - 1)

        fills.append(fill)
        plans.append((peers, shift))
    fills[0]()
    pl.when(mine_block == 0)(lambda: [fill() for fill in fills[1:]] and None)
    for n, (peers, shift) in enumerate(plans):
        if n:
            pl.when(mine_block > 0)(fills[n])
        later = sum(before(my_rank, rank_of(peer)) for peer in peers)

        @pl.when(later > 0)
        def _(n=n, later=later, shift=shift):
            pl.semaphore_wait(ready.at[n + lax.div(shift, 4)], later)

        for peer in peers:
            send(peer)
        if n == len(batches) - 1:
            @pl.when(me > 0)
            def _():
                edge_copy(step_of(me * 0)).start()
    ens_load = pltpu.make_async_copy(ens_hbm, ens, move_sem.at[0])
    ens_load.start()
    arrivals = list(range(tiles))

    def landed(place, sem, first, size):
        part = place.at[max(first, 1) : first + size]
        return pltpu.make_async_copy(part, part, sem)

    def partials(obs, ks, into, base, fresh):
        pert = obs[0:members].astype(F32)
        info = obs[members:].astype(F32)
        obs_weight = info[0:1]
        places = info[2:3] * BASE + info[3:4]
        for k in ks:
            center = float((k - half) * SPACING + SPACING // 2)
            taper = jnp.maximum(1.0 - jnp.abs(places - center) / radius, 0.0)
            rho = taper * taper * obs_weight
            scaled = (pert * rho).astype(BF16)
            part = lax.dot_general(obs, scaled, NT, preferred_element_type=F32)
            if fresh:
                into[k - base] = part
            else:
                into[k - base] += part

    starts = [*range(0, tiles, group), tiles - TAIL]
    for turn, (first, size) in enumerate(zip(starts, [group] * (tiles // group - 1) + [group - TAIL, TAIL])):
        landed(rcv, a2a_recv.at[0, turn], first, size).wait()
        landed(rcv_meta, a2a_recv.at[1, turn], first, size).wait()
        steps = arrivals[first : first + size]
        obs = jnp.concatenate(
            [
                jnp.concatenate([rcv[step] if step else snd[me] for step in steps], axis=1),
                jnp.concatenate(
                    [rcv_meta[step] if step else snd_meta[me] for step in steps], axis=1
                ),
                jnp.zeros((META - META // 4, size * slots), BF16),
            ],
            axis=0,
        )

        def moments(ks, obs=obs, first=first):
            partials(obs, ks, acc, 0, first == 0)

        if first + size < tiles:
            moments(range(points + 2 * half))

    lane = lax.broadcasted_iota(jnp.int32, (members, pair), 1)
    low = lane < members

    def joined(a, b, source=acc):
        return jnp.concatenate([source[a, 0:members], source[b, 0:members]], axis=1)

    def drives_of(a, b, source=acc):
        none = jnp.zeros((1, members), F32)
        return jnp.concatenate(
            [none if k is None else source[k, members + 1 : members + 2] for k in (a, b)], axis=1
        )

    left_copy = pltpu.make_async_remote_copy(
        src_ref=to_left, dst_ref=from_right, send_sem=halo_send.at[0], recv_sem=halo_recv.at[0],
        device_id={"space": lax.rem(me + tiles - 1, tiles)},
    )
    right_copy = pltpu.make_async_remote_copy(
        src_ref=to_right, dst_ref=from_left, send_sem=halo_send.at[1], recv_sem=halo_recv.at[1],
        device_id={"space": lax.rem(me + 1, tiles)},
    )

    fold = members // 2
    extra = members * (half // 4) + fold
    row = lax.broadcasted_iota(jnp.int32, (members, pair), 0)
    within = lax.rem(lane, members)

    def packed(single, ks, source=acc):
        first = [joined(ks[n], ks[n + 1], source) for n in range(0, half, 2)]
        ends = (None, single) if single < ks[0] else (single, None)
        vectors = [drives_of(ks[n], ks[n + 1], source) for n in range(0, half, 2)]
        vectors.append(drives_of(*ends, source))
        vectors += [
            jnp.sum(jnp.where(row == within, other, 0.0), axis=0, keepdims=True)
            for other in first[1::2]
        ]
        spare = -len(vectors) % 8
        if spare:
            vectors.append(jnp.zeros((spare, pair), F32))
        parts = [
            jnp.where(row <= within, first[n], first[n + 1]) for n in range(0, half // 2, 2)
        ]
        tail = jnp.concatenate(
            [source[single, 0:fold], source[single, fold:members]], axis=1
        )
        return jnp.concatenate([*parts, tail, *vectors], axis=0)

    def unpacked(ref):
        pairs = []
        for n in range(half // 4):
            part = ref[n * members : (n + 1) * members]
            flipped = jnp.concatenate([part[:, 0:members].T, part[:, members:].T], axis=1)
            pairs.append(jnp.where(row <= within, part, flipped))
            at = extra + half // 2 + 1 + n
            other = jnp.where(row == within, ref[at : at + 1], flipped)
            pairs.append(jnp.where(row > within, part, other))
        tail = ref[extra - fold : extra]
        corner = tail[:, 0:members].T[fold:]
        bottom = jnp.concatenate([corner, tail[:, members + fold :]], axis=1)
        single = jnp.concatenate([tail[:, 0:members], bottom], axis=0)
        return pairs, single, [ref[extra + n : extra + n + 1] for n in range(half // 2 + 1)]

    last = points + 2 * half - 1
    moments(range(half + 1))
    to_left[...] = packed(0, list(range(1, half + 1)))
    moments(range(last - half, last + 1))
    left_copy.start()
    to_right[...] = packed(last, list(range(last - half, last)))

    moments(range(half + 1, half + 3))

    @pl.when(me < tiles - 1)
    def _():
        right_copy.start()

    moments(range(half + 3, last - half))

    eye = jnp.where(
        lax.rem(lane, members) == lax.broadcasted_iota(jnp.int32, (members, pair), 0), 1.0, 0.0
    )
    mask_low = jnp.where(low, 1.0, 0.0).astype(BF16)
    mask_high = jnp.where(low, 0.0, 1.0).astype(BF16)

    def diagonal(x):
        return jnp.concatenate([x * mask_low, x * mask_high], axis=0)

    def blocks(x):
        hi, lo = halves(x)
        return stationary(diagonal(hi), diagonal(lo))


    count = (points + 2) // 2
    own_pairs = [joined(half - 1 + 2 * i, half + 2 * i) for i in range(count)]
    own_drives = [drives_of(half - 1 + 2 * i, half + 2 * i) for i in range(count)]
    @pl.when(me == 0)
    def _():
        for first in range(0, tiles, group):
            landed(edge_rcv.at[:, 0:sent], edge_recv.at[first // group], first, group).wait()
            near = [
                edge_rcv[step] if step else edge[...] for step in arrivals[first : first + group]
            ]
            partials(
                jnp.concatenate(near, axis=1), range(points + half - 1, points + 2 * half),
                edge_acc, points + half - 1, first == 0,
            )
        from_left[...] = packed(half, list(range(half)), edge_acc)

    left_copy.wait_recv()

    @pl.when(me > 0)
    def _():
        right_copy.wait_recv()

    lefts, left_single, left_drives = unpacked(from_left)
    rights, right_single, right_drives = unpacked(from_right)

    grams = []
    for i in range(count):
        total = own_pairs[i] + (members - 1.0) * eye
        if i < half // 2:
            total = total + lefts[i]
        elif i == half // 2:
            total = total + jnp.concatenate([left_single, right_single], axis=1)
        else:
            total = total + rights[i - half // 2 - 1]
        grams.append(total)
    drives = [
        own_drives[i]
        + (left_drives[i] if i < half // 2 else 0.0)
        + (right_drives[i - half // 2 - 1] if i > half // 2 else 0.0)
        for i in range(count)
    ]
    drives[half // 2] += left_drives[half // 2] + right_drives[half // 2]

    states, scales = [], []
    row_low = lax.broadcasted_iota(jnp.int32, (1, pair), 1) < members
    for total in grams:
        squares = jnp.sum(total * total, axis=0, keepdims=True)
        sum_low = jnp.sum(jnp.where(row_low, squares, 0.0), axis=1, keepdims=True)
        sum_high = jnp.sum(jnp.where(row_low, 0.0, squares), axis=1, keepdims=True)
        scale = jnp.sqrt(jnp.where(row_low, sum_low, sum_high))
        scales.append(scale)
        states.append(total / scale)
    drives = [jnp.broadcast_to(drive, (THIN, pair)) for drive in drives]

    lowers = []
    for sweep in range(NS_ITERS):
        middles = [1.5 * eye - 0.5 * state for state in states]
        weights = [blocks(mid) for mid in middles]
        final = sweep == NS_ITERS - 1
        lefts = [
            ([] if final else [states[i]]) + ([lowers[i]] if sweep else []) + [drives[i]]
            for i in range(count)
        ]
        once = [times(jnp.concatenate(left, axis=0), w) for left, w in zip(lefts, weights)]
        lowers = [x[-THIN - members : -THIN] for x in once] if sweep else middles
        again = [
            x[-THIN:] if final else jnp.concatenate([x[0:members], x[-THIN:]], axis=0)
            for x in once
        ]
        twice = [times(left, w) for left, w in zip(again, weights)]
        states = [x[0:members] for x in twice]
        drives = [x[-THIN:] for x in twice]

    def centered(x):
        sum_low = jnp.sum(jnp.where(low[0:1], x, 0.0), axis=1, keepdims=True)
        sum_high = jnp.sum(jnp.where(low[0:1], 0.0, x), axis=1, keepdims=True)
        return x - jnp.where(low[0:1], sum_low, sum_high) / members

    results = []
    for i in range(count):
        root = lowers[i] / jnp.sqrt(scales[i])
        shift = drives[i][0:1] / scales[i]
        full = math.sqrt(members - 1.0) * root + shift
        results.append(centered(full) + 1.0 / members)
    for i in range(count):
        mine[i] = results[i]
        product[i] = results[i]

    def lag_copy(step):
        return pltpu.make_async_remote_copy(
            src_ref=mine, dst_ref=theirs.at[step - 1],
            send_sem=lag_send.at[step - 1], recv_sem=lag_recv.at[step - 1],
            device_id={"lag": lax.rem(my_lag + lags - step, lags)},
        )

    for step in range(1, lags):
        @pl.when(my_lag >= step)
        def _(step=step):
            lag_copy(step).start()
    for step in range(1, lags):
        @pl.when(my_lag + step < lags)
        def _(step=step):
            lag_copy(step).wait_recv()
            for i in range(count):
                product[i] = times(theirs[step - 1, i], blocks(product[i]))
    for i in range(count):
        both = product[i].astype(BF16)
        turned[i * pair : i * pair + members] = both[:, 0:members]
        turned[i * pair + members : (i + 1) * pair] = both[:, members:]
    ens_load.wait()

    for n, source in enumerate((snd, snd_meta)):
        gone = source.at[1:tiles]
        pltpu.make_async_copy(gone, gone, a2a_send.at[n]).wait()
    left_copy.wait_send()

    @pl.when(me < tiles - 1)
    def _():
        right_copy.wait_send()

    @pl.when(me > 0)
    def _():
        edge_copy(step_of(me * 0)).wait_send()

    for step in range(1, lags):
        @pl.when(my_lag >= step)
        def _(step=step):
            lag_copy(step).wait_send()


def apply_kernel(turned, ens, out_hbm, out, store_sem):
    members, columns = ens.shape
    points = columns // SPACING
    stores = []
    half_span = SPACING // 2
    for s in range(points + 1):
        start = max(s * SPACING - half_span, 0)
        stop = min(s * SPACING + half_span, columns)
        both = jnp.dot(
            turned[s * members : (s + 2) * members], ens[:, start:stop],
            preferred_element_type=F32,
        )
        along = lax.broadcasted_iota(jnp.int32, (1, stop - start), 1).astype(F32)
        second = (along + float(start - (s * SPACING - half_span))) / SPACING
        mixed = both[0:members] * (1.0 - second) + both[members:] * second
        out[:, start:stop] = mixed.astype(BF16)
        if s % 3 == 2:
            first = max((s - 2) * SPACING - half_span, 0)
            store = pltpu.make_async_copy(
                out.at[:, first:stop], out_hbm.at[:, first:stop], store_sem.at[s // 3]
            )
            store.start()
            stores.append(store)
    for store in stores:
        store.wait()


def per_device(ensemble, obs_pert, obs_innov, obs_rinv, obs_tile, obs_column, obs_count):
    members, columns = ensemble.shape[1:]
    own = obs_pert.shape[2]
    tiles, lags = lax.axis_size("space"), lax.axis_size("lag")
    slot_size = max(2, 2 * own // tiles)
    slots = -(-slot_size // LANES) * LANES
    group = 4
    points = columns // SPACING
    half = points // 2
    count = (points + 2) // 2
    pair = 2 * members
    rows = members + META
    vectors = half // 2 + 1 + half // 4
    side = (members * (half // 4) + members // 2 + -(-vectors // 8) * 8, pair)
    turned, held = pl.pallas_call(
        functools.partial(weights_kernel, tiles, lags, slots, group, columns),
        out_shape=(pltpu.VMEM((count * pair, members), BF16), pltpu.VMEM((members, columns), BF16)),
        in_specs=[pl.BlockSpec(memory_space=pltpu.HBM)] * 7,
        out_specs=[pl.BlockSpec(memory_space=pltpu.VMEM)] * 2,
        scratch_shapes=[
            pltpu.SemaphoreType.DMA((1,)),
            pltpu.VMEM((1, own), BF16),
            pltpu.VMEM((1, own), BF16),
            pltpu.VMEM((1, own), jnp.int32),
            pltpu.VMEM((1, own), jnp.int32),
            pltpu.SMEM((1, 1), jnp.int32),
            pltpu.SemaphoreType.DMA((6,)),
            pltpu.VMEM((rows, own), BF16),
            pltpu.VMEM((tiles, members, slots), BF16),
            pltpu.VMEM((tiles, members, slots), BF16),
            pltpu.VMEM((tiles, META // 4, slots), BF16),
            pltpu.VMEM((tiles, META // 4, slots), BF16),
            pltpu.VMEM((points + 2 * half, rows, members), F32),
            pltpu.VMEM(side, F32),
            pltpu.VMEM(side, F32),
            pltpu.VMEM(side, F32),
            pltpu.VMEM(side, F32),
            pltpu.VMEM((count, members, pair), F32),
            pltpu.VMEM((max(lags - 1, 1), count, members, pair), F32),
            pltpu.SemaphoreType.DMA((2,)),
            pltpu.SemaphoreType.DMA((2, tiles // group + 1)),
            pltpu.SemaphoreType.DMA((2,)),
            pltpu.SemaphoreType.DMA((2,)),
            pltpu.SemaphoreType.DMA((max(lags - 1, 1),)),
            pltpu.SemaphoreType.DMA((max(lags - 1, 1),)),
            pltpu.VMEM((count, members, pair), F32),
            pltpu.VMEM((rows, slots), BF16),
            pltpu.VMEM((tiles, rows, slots), BF16),
            pltpu.VMEM((half + 1, rows, members), F32),
            pltpu.SemaphoreType.DMA((1,)),
            pltpu.SemaphoreType.DMA((-(-tiles // group),)),
            pltpu.SemaphoreType.REGULAR((len(batches_of(tiles)),)),
        ],
        compiler_params=pltpu.CompilerParams(
            collective_id=0, has_side_effects=True, vmem_limit_bytes=LIMIT
        ),
        name="ensemble_weights",
    )(*(
        x if x.size == 1 else pltpu.with_memory_space_constraint(x, pltpu.HBM)
        for x in (
            obs_pert[0], obs_innov, obs_rinv, obs_tile[:, :, 0], obs_column, obs_count, ensemble[0]
        )
    ))
    analysis = pl.pallas_call(
        apply_kernel,
        out_shape=jax.ShapeDtypeStruct((members, columns), BF16),
        in_specs=[pl.BlockSpec(memory_space=pltpu.VMEM)] * 2,
        out_specs=pl.BlockSpec(memory_space=pltpu.HBM),
        scratch_shapes=[
            pltpu.VMEM((members, columns), BF16),
            pltpu.SemaphoreType.DMA(((points + 1) // 3,)),
        ],
        compiler_params=pltpu.CompilerParams(vmem_limit_bytes=LIMIT),
        name="apply_weights",
    )(turned, held)
    return analysis[None]


def solution(mesh):
    return jax.shard_map(
        per_device,
        mesh=mesh,
        in_specs=(
            P("lag", None, "space"),
            P("lag", None, "space"),
            P("lag", "space"),
            P("lag", "space"),
            P("lag", "space", None),
            P("lag", "space"),
            P("lag", "space"),
        ),
        out_specs=P("lag", None, "space"),
        check_vma=False,
    )
```
